16 devices in a mesh: fs: 2 (over z), pp: 2 (over y), ep: 4 (over x, core).
Axes of the slice: x: 2, y: 2, z: 2, core: 2. Of those that a mesh axis runs over, the one named last changes fastest.
Arguments:
- w_gate: bfloat16 [2, 32, 2048, 768], P('pp', 'ep', None, 'fs')
- w_up: bfloat16 [2, 32, 2048, 768], P('pp', 'ep', None, 'fs')
- w_down: bfloat16 [2, 32, 768, 2048], P('pp', 'ep', 'fs')
- hot_ids: int32 [4], replicated
Outputs:
- output 1: bfloat16 [2, 32, 2048, 1536], P(None, ('pp', 'ep', 'fs'))
- output 2: bfloat16 [2, 32, 768, 2048], P(None, ('pp', 'ep', 'fs'))
- output 3: bfloat16 [2, 4, 2048, 1536], replicated
- output 4: bfloat16 [2, 4, 768, 2048], replicated
All inputs are finite; a program needn't handle non-finite values.
Results may differ from the reference program's by a relative error of at most 0.001.
Values are sent between devices in bfloat16 or wider.
A program may use at most 1 GiB of HBM per device.

```python
import jax
import jax.numpy as jnp

LAYERS = 2
EXPERTS = 32
D_MODEL = 2048
F_EXPERT = 768
HOT_COUNT = 4


def setup_inputs(seed: int = 0) -> dict:
    root_key = jax.random.key(seed)
    k_gate, k_up, k_down, k_hot = jax.random.split(root_key, 4)
    shape_in = (LAYERS, EXPERTS, D_MODEL, F_EXPERT)
    shape_down = (LAYERS, EXPERTS, F_EXPERT, D_MODEL)
    w_gate = (jax.random.normal(k_gate, shape_in, jnp.float32) * D_MODEL ** -0.5).astype(jnp.bfloat16)
    w_up = (jax.random.normal(k_up, shape_in, jnp.float32) * D_MODEL ** -0.5).astype(jnp.bfloat16)
    w_down = (jax.random.normal(k_down, shape_down, jnp.float32) * F_EXPERT ** -0.5).astype(jnp.bfloat16)
    hot_ids = jax.random.permutation(k_hot, EXPERTS)[:HOT_COUNT].astype(jnp.int32)
    return {"w_gate": w_gate, "w_up": w_up, "w_down": w_down, "hot_ids": hot_ids}


def reference(w_gate, w_up, w_down, hot_ids):
    gate_up = jnp.concatenate([w_gate, w_up], axis=-1)
    hot_gate_up = jnp.take(gate_up, hot_ids, axis=1)
    hot_down = jnp.take(w_down, hot_ids, axis=1)
    return gate_up, w_down, hot_gate_up, hot_down
```

```python
import functools

import jax
import jax.numpy as jnp
from jax import lax
from jax.experimental import pallas as pl
from jax.experimental.pallas import tpu as pltpu
from jax.sharding import PartitionSpec as P

MESH = pl.DeviceIdType.MESH
ANY = pl.BlockSpec(memory_space=pl.ANY)


def pick_kernel(off_ref, g_ref, u_ref, d_ref, pg_ref, pu_ref, pd_ref):
    pg_ref[...] = g_ref[0]
    pu_ref[...] = u_ref[0]
    pd_ref[...] = d_ref[0]


def pick_hot(w_gate, w_up, w_down, offset):
    hot = offset.shape[0]
    _, _, d_model, f_loc = w_gate.shape
    take_in = lambda h, off: (0, off[h], 0, 0)
    put = lambda h, off: (h, 0, 0)
    shape_in = jax.ShapeDtypeStruct((hot, d_model, f_loc), w_gate.dtype)
    shape_down = jax.ShapeDtypeStruct((hot, f_loc, d_model), w_gate.dtype)
    return pl.pallas_call(
        pick_kernel,
        grid_spec=pltpu.PrefetchScalarGridSpec(
            num_scalar_prefetch=1,
            grid=(hot,),
            in_specs=[
                pl.BlockSpec((1, 1, d_model, f_loc), take_in),
                pl.BlockSpec((1, 1, d_model, f_loc), take_in),
                pl.BlockSpec((1, 1, f_loc, d_model), take_in),
            ],
            out_specs=[
                pl.BlockSpec((1, d_model, f_loc), put),
                pl.BlockSpec((1, d_model, f_loc), put),
                pl.BlockSpec((1, f_loc, d_model), put),
            ],
        ),
        out_shape=[shape_in, shape_in, shape_down],
    )(offset, w_gate, w_up, w_down)


def move_kernel(
    owner_ref, wg, wu, wd, pg, pu, pd, o13, o2, h13, h2,
    own13, own2, par13, par2, far13, far2,
    rg_send, rg_recv, loc_sem, dd_send, dd_recv, x_send, x_recv,
    n_send, n_recv, q_send, q_recv, w_sem,
):
    z = lax.axis_index("fs")
    y = lax.axis_index("pp")
    ep = lax.axis_index("ep")
    x, c = ep // 2, ep % 2
    d_model, f_loc = wg.shape[2], wg.shape[3]
    f_all = f_loc * 2
    partner = (z, y, x * 2 + 1 - c)
    x_nbr = (z, y, (1 - x) * 2 + c)
    y_nbr = (z, 1 - y, ep)
    z_nbr = (1 - z, y, ep)

    def cols(half, up):
        return pl.ds(pl.multiple_of(half * f_loc + up * f_all, 128), f_loc)

    def remote(src, dst, send, recv, dev):
        return pltpu.make_async_remote_copy(
            src_ref=src, dst_ref=dst, send_sem=send, recv_sem=recv, device_id=dev, device_id_type=MESH
        )

    def vmem(b13, b2, k):
        return b2.at[k // 3] if k % 3 == 2 else b13.at[(k // 3) * 2 + k % 3]

    def picked(h, w):
        return (pg, pu, pd)[w].at[h]

    def hot_at(h, lay, half, w):
        if w == 2:
            return h2.at[lay, h, pl.ds(pl.multiple_of(half * f_loc, 128), f_loc)]
        return h13.at[lay, h, :, cols(half, w)]

    stays = (x == y) & (c == x)

    def home_refs(j, i, b0, w):
        b1, b2 = (z + i) % 2, (c + j) % 2
        src = (wg, wu, wd)[w].at[0, 4 * b2 + 2 * b1 + b0]
        if w == 2:
            dst = o2.at[y, b0, pl.ds(pl.multiple_of(z * f_loc, 128), f_loc)]
        else:
            dst = o13.at[y, b0, :, cols(z, w)]
        return src, dst, rg_recv.at[w, b0, y * 2 + z], (b1, x, c * 2 + b2)

    def home_copy(j, i, b0, w):
        src, dst, recv, dev = home_refs(j, i, b0, w)
        return remote(src, dst, rg_send.at[w, 4 * j + 2 * i + b0], recv, dev)

    def home_start(j, i, b0, w):
        if (j, i) != (0, 0):
            home_copy(j, i, b0, w).start()
            return

        @pl.when(stays)
        def _():
            src, dst, recv, _ = home_refs(j, i, b0, w)
            pltpu.make_async_copy(src, dst, recv).start()

        @pl.when(jnp.logical_not(stays))
        def _():
            home_copy(j, i, b0, w).start()

    def home_sent(j, i, b0, w):
        if (j, i) != (0, 0):
            home_copy(j, i, b0, w).wait_send()
            return

        @pl.when(jnp.logical_not(stays))
        def _():
            home_copy(j, i, b0, w).wait_send()

    homes = [(j, i, b0, w) for b0 in range(2) for w in range(3) for j in range(2) for i in range(2)]

    CH = range(6)
    dd = [remote(picked(2 * (1 - c) + k // 3, k % 3), vmem(par13, par2, k), dd_send.at[k], dd_recv.at[k], partner) for k in CH]
    own = [pltpu.make_async_copy(picked(2 * c + k // 3, k % 3), vmem(own13, own2, k), loc_sem.at[k]) for k in CH]
    xs = [remote(vmem(own13, own2, k), vmem(far13, far2, k), x_send.at[k], x_recv.at[k], x_nbr) for k in CH]

    def choose(take_a, a, b, out):
        rows = a.shape[0] // 8

        def body(i, carry):
            at = pl.ds(pl.multiple_of(i * rows, 16), rows)
            out[at, :] = jnp.where(take_a, a[at, :], b[at, :])
            return carry

        lax.fori_loop(0, 8, body, 0)

    for k in CH:
        own[k].start()
        dd[k].start()
    for b in homes[:2]:
        home_start(*b)
    for k in CH:
        own[k].wait()
        dd[k].wait_recv()
        owner = owner_ref[2 * c + k // 3]
        choose(owner % 2 == c, vmem(own13, own2, k), vmem(par13, par2, k), vmem(own13, own2, k))
        if k > 0:
            xs[k - 1].start()
    for b in homes[2:4]:
        home_start(*b)
    xs[5].start()
    for b in homes[4:]:
        home_start(*b)

    def hot_of(k):
        return 2 * c + k // 3

    def fan(k):
        src, w = vmem(par13, par2, k), k % 3
        dst = hot_at(hot_of(k), y, z, w)
        return (
            remote(src, dst, n_send.at[0, k], n_recv.at[0, k], y_nbr),
            remote(src, dst, n_send.at[1, k], n_recv.at[1, k], z_nbr),
            remote(src, dst, q_send.at[0, k], q_recv.at[0, k], partner),
            pltpu.make_async_copy(src, dst, w_sem.at[k]),
        )

    def from_y(k):
        at = hot_at(hot_of(k), 1 - y, z, k % 3)
        return at, remote(at, at, q_send.at[1, k], q_recv.at[1, k], partner)

    def from_z(k):
        at = hot_at(hot_of(k), y, 1 - z, k % 3)
        return at, remote(at, at, q_send.at[2, k], q_recv.at[2, k], partner)

    def onward(k):
        if k % 2 == 0:
            at = hot_at(hot_of(k), 1 - y, z, k % 3)
            return remote(at, at, n_send.at[2, k], n_recv.at[2, k], z_nbr)
        at = hot_at(hot_of(k), y, 1 - z, k % 3)
        return remote(at, at, n_send.at[2, k], n_recv.at[2, k], y_nbr)

    def from_diag(k):
        at = hot_at(hot_of(k), 1 - y, 1 - z, k % 3)
        return at, remote(at, at, q_send.at[3, k], q_recv.at[3, k], partner)

    def landed(at, sem):
        pltpu.make_async_copy(at, at, sem).wait()

    for k in CH:
        xs[k].wait_recv()
        owner = owner_ref[2 * c + k // 3]
        choose(owner // 2 == x, vmem(own13, own2, k), vmem(far13, far2, k), vmem(par13, par2, k))
        if k > 0:
            for copy in fan(k - 1):
                copy.start()
    for k in CH:
        xs[k].wait_send()
    for copy in fan(5):
        copy.start()
    for k in CH:
        at, pass_on = from_y(k)
        landed(at, n_recv.at[0, k])
        if k % 2 == 0:
            onward(k).start()
        pass_on.start()
        at, pass_on = from_z(k)
        landed(at, n_recv.at[1, k])
        if k % 2 == 1:
            onward(k).start()
        pass_on.start()
    for k in CH:
        at, pass_on = from_diag(k)
        landed(at, n_recv.at[2, k])
        pass_on.start()

    for k in CH:
        dd[k].wait_send()
        to_y, to_z, to_p, to_self = fan(k)
        to_y.wait_send()
        to_z.wait_send()
        to_p.wait_send()
        to_self.wait()
        onward(k).wait_send()
        from_y(k)[1].wait_send()
        from_z(k)[1].wait_send()
        from_diag(k)[1].wait_send()
    for k in CH:
        h, w = 2 * (1 - c) + k // 3, k % 3
        landed(hot_at(h, y, z, w), q_recv.at[0, k])
        landed(hot_at(h, 1 - y, z, w), q_recv.at[1, k])
        landed(hot_at(h, y, 1 - z, w), q_recv.at[2, k])
        landed(hot_at(h, 1 - y, 1 - z, w), q_recv.at[3, k])
    for b in homes:
        home_sent(*b)
    for w in range(3):
        for b0 in range(2):
            for lay in range(2):
                for half in range(2):
                    if w == 2:
                        at = o2.at[lay, b0, pl.ds(half * f_loc, f_loc)]
                    else:
                        at = o13.at[lay, b0, :, pl.ds(half * f_loc + w * f_all, f_loc)]
                    landed(at, rg_recv.at[w, b0, lay * 2 + half])


def solution(mesh):
    fs_size, pp_size, ep_size = mesh.shape["fs"], mesh.shape["pp"], mesh.shape["ep"]
    in_spec = P("pp", "ep", None, "fs")
    down_spec = P("pp", "ep", "fs", None)
    home_spec = P(None, ("pp", "ep", "fs"), None, None)

    def device_body(w_gate, w_up, w_down, hot_ids):
        dtype = w_gate.dtype
        lay, exp_local, d_model, f_loc = w_gate.shape
        hot = hot_ids.shape[0]
        layers, f_all = lay * pp_size, f_loc * fs_size
        home = exp_local // (fs_size * pp_size)
        offset = jnp.clip(hot_ids - lax.axis_index("ep") * exp_local, 0, exp_local - 1)
        owner = hot_ids // exp_local
        picked = pick_hot(w_gate, w_up, w_down, offset)
        dma = pltpu.SemaphoreType.DMA
        buf13 = pltpu.VMEM((4, d_model, f_loc), dtype)
        buf2 = pltpu.VMEM((2, f_loc, d_model), dtype)
        return pl.pallas_call(
            move_kernel,
            out_shape=[
                jax.ShapeDtypeStruct((layers, home, d_model, 2 * f_all), dtype),
                jax.ShapeDtypeStruct((layers, home, f_all, d_model), dtype),
                jax.ShapeDtypeStruct((layers, hot, d_model, 2 * f_all), dtype),
                jax.ShapeDtypeStruct((layers, hot, f_all, d_model), dtype),
            ],
            in_specs=[pl.BlockSpec(memory_space=pltpu.SMEM)] + [ANY] * 6,
            out_specs=[ANY] * 4,
            scratch_shapes=[
                buf13, buf2, buf13, buf2, buf13, buf2,
                dma((3, 8)), dma((3, 2, 4)), dma((6,)), dma((6,)), dma((6,)), dma((6,)), dma((6,)),
                dma((3, 6)), dma((3, 6)), dma((4, 6)), dma((4, 6)), dma((6,)),
            ],
            compiler_params=pltpu.CompilerParams(has_side_effects=True, vmem_limit_bytes=48 * 1024 * 1024),
        )(owner, w_gate, w_up, w_down, *picked)

    return jax.shard_map(
        device_body,
        mesh=mesh,
        in_specs=(in_spec, in_spec, down_spec, P()),
        out_specs=(home_spec, home_spec, P(), P()),
        check_vma=False,
    )
```

```python
import functools

import jax
import jax.numpy as jnp
from jax import lax
from jax.experimental import pallas as pl
from jax.experimental.pallas import tpu as pltpu
from jax.sharding import PartitionSpec as P

MESH = pl.DeviceIdType.MESH
ANY = pl.BlockSpec(memory_space=pl.ANY)


def pick_kernel(off_ref, g_ref, u_ref, d_ref, pg_ref, pu_ref, pd_ref):
    pg_ref[...] = g_ref[0]
    pu_ref[...] = u_ref[0]
    pd_ref[...] = d_ref[0]


def pick_hot(w_gate, w_up, w_down, offset):
    hot = offset.shape[0]
    _, _, d_model, f_loc = w_gate.shape
    take_in = lambda h, off: (0, off[h], 0, 0)
    put = lambda h, off: (h, 0, 0)
    shape_in = jax.ShapeDtypeStruct((hot, d_model, f_loc), w_gate.dtype)
    shape_down = jax.ShapeDtypeStruct((hot, f_loc, d_model), w_gate.dtype)
    return pl.pallas_call(
        pick_kernel,
        grid_spec=pltpu.PrefetchScalarGridSpec(
            num_scalar_prefetch=1,
            grid=(hot,),
            in_specs=[
                pl.BlockSpec((1, 1, d_model, f_loc), take_in),
                pl.BlockSpec((1, 1, d_model, f_loc), take_in),
                pl.BlockSpec((1, 1, f_loc, d_model), take_in),
            ],
            out_specs=[
                pl.BlockSpec((1, d_model, f_loc), put),
                pl.BlockSpec((1, d_model, f_loc), put),
                pl.BlockSpec((1, f_loc, d_model), put),
            ],
        ),
        out_shape=[shape_in, shape_in, shape_down],
    )(offset, w_gate, w_up, w_down)


def move_kernel(
    owner_ref, wg, wu, wd, pg, pu, pd, o13, o2, h13, h2,
    own13, own2, par13, par2, far13, far2,
    rg_send, rg_recv, loc_sem, dd_send, dd_recv, x_send, x_recv,
    n_send, n_recv, f_send, q_send, q_recv, w_sem,
):
    z = lax.axis_index("fs")
    y = lax.axis_index("pp")
    ep = lax.axis_index("ep")
    x, c = ep // 2, ep % 2
    d_model, f_loc = wg.shape[2], wg.shape[3]
    f_all = f_loc * 2
    partner = (z, y, x * 2 + 1 - c)
    x_nbr = (z, y, (1 - x) * 2 + c)
    y_nbr = (z, 1 - y, ep)
    z_nbr = (1 - z, y, ep)

    def cols(half, up):
        return pl.ds(pl.multiple_of(half * f_loc + up * f_all, 128), f_loc)

    def remote(src, dst, send, recv, dev):
        return pltpu.make_async_remote_copy(
            src_ref=src, dst_ref=dst, send_sem=send, recv_sem=recv, device_id=dev, device_id_type=MESH
        )

    def vmem(b13, b2, k):
        return b2.at[k // 3] if k % 3 == 2 else b13.at[(k // 3) * 2 + k % 3]

    def picked(h, w):
        return (pg, pu, pd)[w].at[h]

    def hot_at(h, lay, half, w):
        if w == 2:
            return h2.at[lay, h, pl.ds(pl.multiple_of(half * f_loc, 128), f_loc)]
        return h13.at[lay, h, :, cols(half, w)]

    stays = (x == y) & (c == x)

    def home_refs(j, i, b0, w):
        b1, b2 = (z + i) % 2, (c + j) % 2
        src = (wg, wu, wd)[w].at[0, 4 * b2 + 2 * b1 + b0]
        if w == 2:
            dst = o2.at[y, b0, pl.ds(pl.multiple_of(z * f_loc, 128), f_loc)]
        else:
            dst = o13.at[y, b0, :, cols(z, w)]
        return src, dst, rg_recv.at[w, b0, y * 2 + z], (b1, x, c * 2 + b2)

    def home_copy(j, i, b0, w):
        src, dst, recv, dev = home_refs(j, i, b0, w)
        return remote(src, dst, rg_send.at[w, 4 * j + 2 * i + b0], recv, dev)

    def home_start(j, i, b0, w):
        if (j, i) != (0, 0):
            home_copy(j, i, b0, w).start()
            return

        @pl.when(stays)
        def _():
            src, dst, recv, _ = home_refs(j, i, b0, w)
            pltpu.make_async_copy(src, dst, recv).start()

        @pl.when(jnp.logical_not(stays))
        def _():
            home_copy(j, i, b0, w).start()

    def home_sent(j, i, b0, w):
        if (j, i) != (0, 0):
            home_copy(j, i, b0, w).wait_send()
            return

        @pl.when(jnp.logical_not(stays))
        def _():
            home_copy(j, i, b0, w).wait_send()

    homes = [(j, i, b0, w) for b0 in range(2) for w in range(3) for j in range(2) for i in range(2)]

    waiting = list(homes)

    def issue(count):
        for _ in range(count):
            home_start(*waiting.pop(0))

    CH = range(6)
    dd = [remote(picked(2 * (1 - c) + k // 3, k % 3), vmem(par13, par2, k), dd_send.at[k], dd_recv.at[k], partner) for k in CH]
    own = [pltpu.make_async_copy(picked(2 * c + k // 3, k % 3), vmem(own13, own2, k), loc_sem.at[k]) for k in CH]
    xs = [remote(vmem(own13, own2, k), vmem(far13, far2, k), x_send.at[k], x_recv.at[k], x_nbr) for k in CH]

    def choose(take_a, a, b, out):
        rows = a.shape[0] // 8

        def body(i, carry):
            at = pl.ds(pl.multiple_of(i * rows, 16), rows)
            out[at, :] = jnp.where(take_a, a[at, :], b[at, :])
            return carry

        lax.fori_loop(0, 8, body, 0)

    for k in CH:
        own[k].start()
        dd[k].start()
    issue(2)
    for k in CH:
        own[k].wait()
        dd[k].wait_recv()
        owner = owner_ref[2 * c + k // 3]
        choose(owner % 2 == c, vmem(own13, own2, k), vmem(par13, par2, k), vmem(own13, own2, k))
        if k > 0:
            xs[k - 1].start()
    issue(1)
    xs[5].start()
    issue(3)

    def hot_of(k):
        return 2 * c + k // 3

    def fan(k):
        src, w = vmem(par13, par2, k), k % 3
        dst = hot_at(hot_of(k), y, z, w)
        return (
            remote(src, dst, n_send.at[0, k], n_recv.at[0, k], y_nbr),
            remote(src, dst, n_send.at[1, k], n_recv.at[1, k], z_nbr),
            remote(src, dst, q_send.at[0, k], q_recv.at[0, k], partner),
            pltpu.make_async_copy(src, dst, w_sem.at[k]),
        )

    def from_y(k):
        at = hot_at(hot_of(k), 1 - y, z, k % 3)
        return at, remote(at, at, q_send.at[1, k], q_recv.at[1, k], partner)

    def from_z(k):
        at = hot_at(hot_of(k), y, 1 - z, k % 3)
        return at, remote(at, at, q_send.at[2, k], q_recv.at[2, k], partner)

    def onward(k):
        if k % 2 == 0:
            at = hot_at(hot_of(k), 1 - y, z, k % 3)
            return remote(at, at, n_send.at[2, k], n_recv.at[2, k], z_nbr)
        at = hot_at(hot_of(k), y, 1 - z, k % 3)
        return remote(at, at, n_send.at[2, k], n_recv.at[2, k], y_nbr)

    def from_diag(k):
        at = hot_at(hot_of(k), 1 - y, 1 - z, k % 3)
        return at, remote(at, at, q_send.at[3, k], q_recv.at[3, k], partner)

    def landed(at, sem):
        pltpu.make_async_copy(at, at, sem).wait()

    def comes_here(k):
        return x == k // 2

    def across(k):
        at = hot_at(hot_of(k), 1 - y, 1 - z, k % 3)
        return remote(at, at, f_send.at[k], n_recv.at[2, k], x_nbr)

    def onward_do(k, what):
        if k < 4:
            pl.when(comes_here(k))(lambda: what(onward(k)))
        else:
            what(onward(k))

    for s in range(10):
        if s < 6:
            xs[s].wait_recv()
            owner = owner_ref[2 * c + s // 3]
            choose(owner // 2 == x, vmem(own13, own2, s), vmem(far13, far2, s), vmem(par13, par2, s))
        if 1 <= s <= 6:
            for copy in fan(s - 1):
                copy.start()
        if s < 9:
            issue(2)
        k = s - 2
        if 0 <= k < 6:
            at, pass_on = from_y(k)
            landed(at, n_recv.at[0, k])
            if k % 2 == 0:
                onward_do(k, lambda copy: copy.start())
            pass_on.start()
            at, pass_on = from_z(k)
            landed(at, n_recv.at[1, k])
            if k % 2 == 1:
                onward_do(k, lambda copy: copy.start())
            pass_on.start()
        k = s - 4
        if 0 <= k < 6:
            at, pass_on = from_diag(k)
            landed(at, n_recv.at[2, k])
            if k < 4:
                pl.when(comes_here(k))(lambda: across(k).start())
            pass_on.start()

    for k in CH:
        dd[k].wait_send()
        to_y, to_z, to_p, to_self = fan(k)
        to_y.wait_send()
        to_z.wait_send()
        to_p.wait_send()
        to_self.wait()
        xs[k].wait_send()
        onward_do(k, lambda copy: copy.wait_send())
        if k < 4:
            pl.when(comes_here(k))(lambda: across(k).wait_send())
        from_y(k)[1].wait_send()
        from_z(k)[1].wait_send()
        from_diag(k)[1].wait_send()
    for k in CH:
        h, w = 2 * (1 - c) + k // 3, k % 3
        landed(hot_at(h, y, z, w), q_recv.at[0, k])
        landed(hot_at(h, 1 - y, z, w), q_recv.at[1, k])
        landed(hot_at(h, y, 1 - z, w), q_recv.at[2, k])
        landed(hot_at(h, 1 - y, 1 - z, w), q_recv.at[3, k])
    for b in homes:
        home_sent(*b)
    for w in range(3):
        for b0 in range(2):
            for lay in range(2):
                for half in range(2):
                    if w == 2:
                        at = o2.at[lay, b0, pl.ds(half * f_loc, f_loc)]
                    else:
                        at = o13.at[lay, b0, :, pl.ds(half * f_loc + w * f_all, f_loc)]
                    landed(at, rg_recv.at[w, b0, lay * 2 + half])


def solution(mesh):
    fs_size, pp_size, ep_size = mesh.shape["fs"], mesh.shape["pp"], mesh.shape["ep"]
    in_spec = P("pp", "ep", None, "fs")
    down_spec = P("pp", "ep", "fs", None)
    home_spec = P(None, ("pp", "ep", "fs"), None, None)

    def device_body(w_gate, w_up, w_down, hot_ids):
        dtype = w_gate.dtype
        lay, exp_local, d_model, f_loc = w_gate.shape
        hot = hot_ids.shape[0]
        layers, f_all = lay * pp_size, f_loc * fs_size
        home = exp_local // (fs_size * pp_size)
        offset = jnp.clip(hot_ids - lax.axis_index("ep") * exp_local, 0, exp_local - 1)
        owner = hot_ids // exp_local
        picked = pick_hot(w_gate, w_up, w_down, offset)
        dma = pltpu.SemaphoreType.DMA
        buf13 = pltpu.VMEM((4, d_model, f_loc), dtype)
        buf2 = pltpu.VMEM((2, f_loc, d_model), dtype)
        return pl.pallas_call(
            move_kernel,
            out_shape=[
                jax.ShapeDtypeStruct((layers, home, d_model, 2 * f_all), dtype),
                jax.ShapeDtypeStruct((layers, home, f_all, d_model), dtype),
                jax.ShapeDtypeStruct((layers, hot, d_model, 2 * f_all), dtype),
                jax.ShapeDtypeStruct((layers, hot, f_all, d_model), dtype),
            ],
            in_specs=[pl.BlockSpec(memory_space=pltpu.SMEM)] + [ANY] * 6,
            out_specs=[ANY] * 4,
            scratch_shapes=[
                buf13, buf2, buf13, buf2, buf13, buf2,
                dma((3, 8)), dma((3, 2, 4)), dma((6,)), dma((6,)), dma((6,)), dma((6,)), dma((6,)),
                dma((3, 6)), dma((3, 6)), dma((4,)), dma((4, 6)), dma((4, 6)), dma((6,)),
            ],
            compiler_params=pltpu.CompilerParams(has_side_effects=True, vmem_limit_bytes=48 * 1024 * 1024),
        )(owner, w_gate, w_up, w_down, *picked)

    return jax.shard_map(
        device_body,
        mesh=mesh,
        in_specs=(in_spec, in_spec, down_spec, P()),
        out_specs=(home_spec, home_spec, P(), P()),
        check_vma=False,
    )
```

```python
import functools

import jax
import jax.numpy as jnp
from jax import lax
from jax.experimental import pallas as pl
from jax.experimental.pallas import tpu as pltpu
from jax.sharding import PartitionSpec as P

MESH = pl.DeviceIdType.MESH
ANY = pl.BlockSpec(memory_space=pl.ANY)


def pick_kernel(off_ref, g_ref, u_ref, d_ref, pg_ref, pu_ref, pd_ref):
    pg_ref[...] = g_ref[0]
    pu_ref[...] = u_ref[0]
    pd_ref[...] = d_ref[0]


def pick_hot(w_gate, w_up, w_down, offset):
    hot = offset.shape[0]
    _, _, d_model, f_loc = w_gate.shape
    take_in = lambda h, off: (0, off[h], 0, 0)
    put = lambda h, off: (h, 0, 0)
    shape_in = jax.ShapeDtypeStruct((hot, d_model, f_loc), w_gate.dtype)
    shape_down = jax.ShapeDtypeStruct((hot, f_loc, d_model), w_gate.dtype)
    return pl.pallas_call(
        pick_kernel,
        grid_spec=pltpu.PrefetchScalarGridSpec(
            num_scalar_prefetch=1,
            grid=(hot,),
            in_specs=[
                pl.BlockSpec((1, 1, d_model, f_loc), take_in),
                pl.BlockSpec((1, 1, d_model, f_loc), take_in),
                pl.BlockSpec((1, 1, f_loc, d_model), take_in),
            ],
            out_specs=[
                pl.BlockSpec((1, d_model, f_loc), put),
                pl.BlockSpec((1, d_model, f_loc), put),
                pl.BlockSpec((1, f_loc, d_model), put),
            ],
        ),
        out_shape=[shape_in, shape_in, shape_down],
    )(offset, w_gate, w_up, w_down)


def move_kernel(
    owner_ref, wg, wu, wd, pg, pu, pd, o13, o2, h13, h2, t0, t1, t2, t3,
    own13, own2, par13, par2, far13, far2, held, t_sem,
    rg_send, rg_recv, loc_sem, dd_send, dd_recv, x_send, x_recv,
    n_send, n_recv, q_send, q_recv, w_sem,
):
    z = lax.axis_index("fs")
    y = lax.axis_index("pp")
    ep = lax.axis_index("ep")
    x, c = ep // 2, ep % 2
    d_model, f_loc = wg.shape[2], wg.shape[3]
    f_all = f_loc * 2
    partner = (z, y, x * 2 + 1 - c)
    x_nbr = (z, y, (1 - x) * 2 + c)
    y_nbr = (z, 1 - y, ep)
    z_nbr = (1 - z, y, ep)

    def cols(half, up):
        return pl.ds(pl.multiple_of(half * f_loc + up * f_all, 128), f_loc)

    def remote(src, dst, send, recv, dev):
        return pltpu.make_async_remote_copy(
            src_ref=src, dst_ref=dst, send_sem=send, recv_sem=recv, device_id=dev, device_id_type=MESH
        )

    def vmem(b13, b2, k):
        return b2.at[k // 3] if k % 3 == 2 else b13.at[(k // 3) * 2 + k % 3]

    def picked(h, w):
        return (pg, pu, pd)[w].at[h]

    def hot_at(h, lay, half, w):
        if w == 2:
            return h2.at[lay, h, pl.ds(pl.multiple_of(half * f_loc, 128), f_loc)]
        return h13.at[lay, h, :, cols(half, w)]

    stays = (x == y) & (c == x)

    def home_refs(j, i, b0, w):
        b1, b2 = (z + i) % 2, (c + j) % 2
        src = (wg, wu, wd)[w].at[0, 4 * b2 + 2 * b1 + b0]
        if w == 2:
            dst = o2.at[y, pl.ds(pl.multiple_of(z * f_loc, 128), f_loc)]
        else:
            dst = o13.at[y, b0, :, cols(z, w)]
        return src, dst, rg_recv.at[w, b0, y * 2 + z], (b1, x, c * 2 + b2)

    def home_copy(j, i, b0, w):
        src, dst, recv, dev = home_refs(j, i, b0, w)
        return remote(src, dst, rg_send.at[w, 4 * j + 2 * i + b0], recv, dev)

    def home_start(j, i, b0, w):
        if (j, i) != (0, 0):
            home_copy(j, i, b0, w).start()
            return

        @pl.when(stays)
        def _():
            src, dst, recv, _ = home_refs(j, i, b0, w)
            pltpu.make_async_copy(src, dst, recv).start()

        @pl.when(jnp.logical_not(stays))
        def _():
            home_copy(j, i, b0, w).start()

    def home_sent(j, i, b0, w):
        if (j, i) != (0, 0):
            home_copy(j, i, b0, w).wait_send()
            return

        @pl.when(jnp.logical_not(stays))
        def _():
            home_copy(j, i, b0, w).wait_send()

    homes = [
        (j, i, b0, w)
        for b0 in range(2) for w in range(3) for j in range(2) for i in range(2) if (b0, w) != (1, 2)
    ]

    tails = []
    for n in range(4):
        e = 4 * ((c + y + n % 2) % 2) + 2 * ((z + n // 2) % 2) + 1
        tails.append((
            pltpu.make_async_copy(wd.at[0, e], held.at[n], t_sem.at[0, n]),
            pltpu.make_async_copy(held.at[n], (t0, t1, t2, t3)[n], t_sem.at[1, n]),
        ))

    CH = range(6)
    dd = [remote(picked(2 * (1 - c) + k // 3, k % 3), vmem(par13, par2, k), dd_send.at[k], dd_recv.at[k], partner) for k in CH]
    own = [pltpu.make_async_copy(picked(2 * c + k // 3, k % 3), vmem(own13, own2, k), loc_sem.at[k]) for k in CH]
    xs = [remote(vmem(own13, own2, k), vmem(far13, far2, k), x_send.at[k], x_recv.at[k], x_nbr) for k in CH]

    def choose(take_a, a, b, out):
        rows = a.shape[0] // 8

        def body(i, carry):
            at = pl.ds(pl.multiple_of(i * rows, 16), rows)
            out[at, :] = jnp.where(take_a, a[at, :], b[at, :])
            return carry

        lax.fori_loop(0, 8, body, 0)

    for k in CH:
        own[k].start()
        dd[k].start()
    for b in homes[:2]:
        home_start(*b)
    for k in CH:
        own[k].wait()
        dd[k].wait_recv()
        owner = owner_ref[2 * c + k // 3]
        choose(owner % 2 == c, vmem(own13, own2, k), vmem(par13, par2, k), vmem(own13, own2, k))
        if k > 0:
            xs[k - 1].start()
    for b in homes[2:4]:
        home_start(*b)
    xs[5].start()
    for b in homes[4:]:
        home_start(*b)

    def hot_of(k):
        return 2 * c + k // 3

    def fan(k):
        src, w = vmem(par13, par2, k), k % 3
        dst = hot_at(hot_of(k), y, z, w)
        return (
            remote(src, dst, n_send.at[0, k], n_recv.at[0, k], y_nbr),
            remote(src, dst, n_send.at[1, k], n_recv.at[1, k], z_nbr),
            remote(src, dst, q_send.at[0, k], q_recv.at[0, k], partner),
            pltpu.make_async_copy(src, dst, w_sem.at[k]),
        )

    def from_y(k):
        at = hot_at(hot_of(k), 1 - y, z, k % 3)
        return at, remote(at, at, q_send.at[1, k], q_recv.at[1, k], partner)

    def from_z(k):
        at = hot_at(hot_of(k), y, 1 - z, k % 3)
        return at, remote(at, at, q_send.at[2, k], q_recv.at[2, k], partner)

    def onward(k):
        if k % 2 == 0:
            at = hot_at(hot_of(k), 1 - y, z, k % 3)
            return remote(at, at, n_send.at[2, k], n_recv.at[2, k], z_nbr)
        at = hot_at(hot_of(k), y, 1 - z, k % 3)
        return remote(at, at, n_send.at[2, k], n_recv.at[2, k], y_nbr)

    def from_diag(k):
        at = hot_at(hot_of(k), 1 - y, 1 - z, k % 3)
        return at, remote(at, at, q_send.at[3, k], q_recv.at[3, k], partner)

    def landed(at, sem):
        pltpu.make_async_copy(at, at, sem).wait()

    for load, _ in tails:
        load.start()
    for load, store in tails:
        load.wait()
        store.start()
    for k in CH:
        xs[k].wait_recv()
        owner = owner_ref[2 * c + k // 3]
        choose(owner // 2 == x, vmem(own13, own2, k), vmem(far13, far2, k), vmem(par13, par2, k))
        if k > 0:
            for copy in fan(k - 1):
                copy.start()
    for k in CH:
        xs[k].wait_send()
    for copy in fan(5):
        copy.start()
    for k in CH:
        at, pass_on = from_y(k)
        landed(at, n_recv.at[0, k])
        if k % 2 == 0:
            onward(k).start()
        pass_on.start()
        at, pass_on = from_z(k)
        landed(at, n_recv.at[1, k])
        if k % 2 == 1:
            onward(k).start()
        pass_on.start()
    for k in CH:
        at, pass_on = from_diag(k)
        landed(at, n_recv.at[2, k])
        pass_on.start()

    for _, store in tails:
        store.wait()
    for k in CH:
        dd[k].wait_send()
        to_y, to_z, to_p, to_self = fan(k)
        to_y.wait_send()
        to_z.wait_send()
        to_p.wait_send()
        to_self.wait()
        onward(k).wait_send()
        from_y(k)[1].wait_send()
        from_z(k)[1].wait_send()
        from_diag(k)[1].wait_send()
    for k in CH:
        h, w = 2 * (1 - c) + k // 3, k % 3
        landed(hot_at(h, y, z, w), q_recv.at[0, k])
        landed(hot_at(h, 1 - y, z, w), q_recv.at[1, k])
        landed(hot_at(h, y, 1 - z, w), q_recv.at[2, k])
        landed(hot_at(h, 1 - y, 1 - z, w), q_recv.at[3, k])
    for b in homes:
        home_sent(*b)
    for w in range(3):
        for b0 in range(1 if w == 2 else 2):
            for lay in range(2):
                for half in range(2):
                    if w == 2:
                        at = o2.at[lay, pl.ds(half * f_loc, f_loc)]
                    else:
                        at = o13.at[lay, b0, :, pl.ds(half * f_loc + w * f_all, f_loc)]
                    landed(at, rg_recv.at[w, b0, lay * 2 + half])


def settle_kernel(o13, o2, h13, h2, q13, q2, g13, g2, buf13, buf2, sems):
    slots = buf13.shape[0]
    rows13, rows2 = buf13.shape[1], buf2.shape[1]

    def tiles(src, dst, rows, buf):
        return [
            (src.at[pl.ds(r, rows)], dst.at[pl.ds(r, rows)], buf) for r in range(0, src.shape[0], rows)
        ]

    work = []
    for lay in range(2):
        for n in range(o13.shape[1]):
            work += tiles(o13.at[lay, n], q13.at[lay, n], rows13, buf13)
        work += tiles(o2.at[lay], q2.at[lay, 0], rows2, buf2)
        for n in range(h13.shape[1]):
            work += tiles(h13.at[lay, n], g13.at[lay, n], rows13, buf13)
            work += tiles(h2.at[lay, n], g2.at[lay, n], rows2, buf2)

    used = {id(buf13): 0, id(buf2): 0}
    steps = []
    last = {}
    for src, dst, buf in work:
        kind = 0 if buf is buf13 else 1
        slot = used[id(buf)] % slots
        used[id(buf)] += 1
        before = last.get((kind, slot))
        step = (
            pltpu.make_async_copy(src, buf.at[slot], sems.at[kind, 0, slot]),
            pltpu.make_async_copy(buf.at[slot], dst, sems.at[kind, 1, slot]),
            before,
        )
        last[kind, slot] = step
        steps.append(step)
    lag = slots // 2
    for n in range(len(steps) + lag):
        if n < len(steps):
            load, _, before = steps[n]
            if before is not None:
                before[1].wait()
            load.start()
        if n >= lag:
            load, store, _ = steps[n - lag]
            load.wait()
            store.start()
    for step in last.values():
        step[1].wait()


def place_kernel(t0, t1, r0, r1, r2, r3, q2_in, q2, buf, sems):
    z = lax.axis_index("fs")
    y = lax.axis_index("pp")
    ep = lax.axis_index("ep")
    x, c = ep // 2, ep % 2
    f_loc = buf.shape[1]

    def each(n, what):
        source = (r0, r1, r2, r3)[n]
        if n >= 2:
            what(source)
            return
        here = (x == y) & (c == x) & (y == n)
        pl.when(here)(lambda: what((t0, t1)[n]))
        pl.when(jnp.logical_not(here))(lambda: what(source))

    def store(n):
        lay, half = (c + x + n % 2) % 2, (z + n // 2) % 2
        rows = pl.ds(pl.multiple_of(half * f_loc, 128), f_loc)
        return pltpu.make_async_copy(buf.at[n], q2.at[lay, 1, rows], sems.at[1, n])

    for n in range(4):
        each(n, lambda src: pltpu.make_async_copy(src, buf.at[n], sems.at[0, n]).start())
    for n in range(4):
        pltpu.make_async_copy(r0, buf.at[n], sems.at[0, n]).wait()
        store(n).start()
    for n in range(4):
        store(n).wait()


def solution(mesh):
    fs_size, pp_size, ep_size = mesh.shape["fs"], mesh.shape["pp"], mesh.shape["ep"]
    in_spec = P("pp", "ep", None, "fs")
    down_spec = P("pp", "ep", "fs", None)
    home_spec = P(None, ("pp", "ep", "fs"), None, None)

    def tail_pairs(n):
        pairs = []
        for z in range(fs_size):
            for y in range(pp_size):
                for ep in range(ep_size):
                    x, c = ep // 2, ep % 2
                    b1, b2 = (z + n // 2) % 2, (c + y + n % 2) % 2
                    src = (z * pp_size + y) * ep_size + ep
                    dst = (b1 * pp_size + x) * ep_size + c * 2 + b2
                    if src != dst:
                        pairs.append((src, dst))
        return pairs

    def device_body(w_gate, w_up, w_down, hot_ids):
        dtype = w_gate.dtype
        lay, exp_local, d_model, f_loc = w_gate.shape
        hot = hot_ids.shape[0]
        layers, f_all = lay * pp_size, f_loc * fs_size
        home = exp_local // (fs_size * pp_size)
        offset = jnp.clip(hot_ids - lax.axis_index("ep") * exp_local, 0, exp_local - 1)
        owner = hot_ids // exp_local
        picked = pick_hot(w_gate, w_up, w_down, offset)
        dma = pltpu.SemaphoreType.DMA
        buf13 = pltpu.VMEM((4, d_model, f_loc), dtype)
        buf2 = pltpu.VMEM((2, f_loc, d_model), dtype)
        shape = lambda *dims: jax.ShapeDtypeStruct(dims, dtype)
        held = pltpu.VMEM((4, f_loc, d_model), dtype)
        o13, o2, h13, h2, *tail = pl.pallas_call(
            move_kernel,
            out_shape=[
                shape(layers, home, d_model, 2 * f_all),
                shape(layers, f_all, d_model),
                shape(layers, hot, d_model, 2 * f_all),
                shape(layers, hot, f_all, d_model),
            ] + [shape(f_loc, d_model)] * 4,
            in_specs=[pl.BlockSpec(memory_space=pltpu.SMEM)] + [ANY] * 6,
            out_specs=[ANY] * 8,
            scratch_shapes=[
                buf13, buf2, buf13, buf2, buf13, buf2, held, dma((2, 4)),
                dma((3, 8)), dma((3, 2, 4)), dma((6,)), dma((6,)), dma((6,)), dma((6,)), dma((6,)),
                dma((3, 6)), dma((3, 6)), dma((4, 6)), dma((4, 6)), dma((6,)),
            ],
            compiler_params=pltpu.CompilerParams(has_side_effects=True, vmem_limit_bytes=48 * 1024 * 1024),
        )(owner, w_gate, w_up, w_down, *picked)
        moved = [lax.ppermute(t, ("fs", "pp", "ep"), tail_pairs(n)) for n, t in enumerate(tail)]
        copied = 4 * (o13.size + o2.size + h13.size + h2.size)
        q13, q2, g13, g2 = pl.pallas_call(
            settle_kernel,
            out_shape=[
                shape(*o13.shape), shape(layers, home, f_all, d_model), shape(*h13.shape), shape(*h2.shape),
            ],
            in_specs=[ANY] * 4,
            out_specs=[ANY] * 4,
            scratch_shapes=[
                pltpu.VMEM((12, 512, 2 * f_all), dtype), pltpu.VMEM((12, f_loc, d_model), dtype), dma((2, 2, 12)),
            ],
            cost_estimate=pl.CostEstimate(flops=10**9, bytes_accessed=copied, transcendentals=0),
            compiler_params=pltpu.CompilerParams(vmem_limit_bytes=48 * 1024 * 1024),
        )(o13, o2, h13, h2)
        q2 = pl.pallas_call(
            place_kernel,
            out_shape=shape(*q2.shape),
            in_specs=[ANY] * 7,
            out_specs=ANY,
            scratch_shapes=[held, dma((2, 4))],
            input_output_aliases={6: 0},
            compiler_params=pltpu.CompilerParams(vmem_limit_bytes=56 * 1024 * 1024),
        )(tail[0], tail[1], *moved, q2)
        return q13, q2, g13, g2

    return jax.shard_map(
        device_body,
        mesh=mesh,
        in_specs=(in_spec, in_spec, down_spec, P()),
        out_specs=(home_spec, home_spec, P(), P()),
        check_vma=False,
    )
```

```python
import functools

import jax
import jax.numpy as jnp
from jax import lax
from jax.experimental import pallas as pl
from jax.experimental.pallas import tpu as pltpu
from jax.sharding import PartitionSpec as P

MESH = pl.DeviceIdType.MESH
ANY = pl.BlockSpec(memory_space=pl.ANY)


def pick_kernel(off_ref, g_ref, u_ref, d_ref, pg_ref, pu_ref, pd_ref):
    pg_ref[...] = g_ref[0]
    pu_ref[...] = u_ref[0]
    pd_ref[...] = d_ref[0]


def pick_hot(w_gate, w_up, w_down, offset):
    hot = offset.shape[0]
    _, _, d_model, f_loc = w_gate.shape
    take_in = lambda h, off: (0, off[h], 0, 0)
    put = lambda h, off: (h, 0, 0)
    shape_in = jax.ShapeDtypeStruct((hot, d_model, f_loc), w_gate.dtype)
    shape_down = jax.ShapeDtypeStruct((hot, f_loc, d_model), w_gate.dtype)
    return pl.pallas_call(
        pick_kernel,
        grid_spec=pltpu.PrefetchScalarGridSpec(
            num_scalar_prefetch=1,
            grid=(hot,),
            in_specs=[
                pl.BlockSpec((1, 1, d_model, f_loc), take_in),
                pl.BlockSpec((1, 1, d_model, f_loc), take_in),
                pl.BlockSpec((1, 1, f_loc, d_model), take_in),
            ],
            out_specs=[
                pl.BlockSpec((1, d_model, f_loc), put),
                pl.BlockSpec((1, d_model, f_loc), put),
                pl.BlockSpec((1, f_loc, d_model), put),
            ],
        ),
        out_shape=[shape_in, shape_in, shape_down],
    )(offset, w_gate, w_up, w_down)


def move_kernel(
    owner_ref, wg, wu, wd, pg, pu, pd, o13, o2, o2b, h13, h2, t0, t1, t2, t3,
    own13, own2, par13, par2, far13, far2, held, t_sem,
    rg_send, rg_recv, loc_sem, dd_send, dd_recv, x_send, x_recv,
    n_send, n_recv, f_send, q_send, q_recv, w_sem,
):
    z = lax.axis_index("fs")
    y = lax.axis_index("pp")
    ep = lax.axis_index("ep")
    x, c = ep // 2, ep % 2
    d_model, f_loc = wg.shape[2], wg.shape[3]
    f_all = f_loc * 2
    tail_rows = t0.shape[0]
    kept = f_loc - tail_rows
    partner = (z, y, x * 2 + 1 - c)
    x_nbr = (z, y, (1 - x) * 2 + c)
    y_nbr = (z, 1 - y, ep)
    z_nbr = (1 - z, y, ep)

    def cols(half, up):
        return pl.ds(pl.multiple_of(half * f_loc + up * f_all, 128), f_loc)

    def remote(src, dst, send, recv, dev):
        return pltpu.make_async_remote_copy(
            src_ref=src, dst_ref=dst, send_sem=send, recv_sem=recv, device_id=dev, device_id_type=MESH
        )

    def vmem(b13, b2, k):
        return b2.at[k // 3] if k % 3 == 2 else b13.at[(k // 3) * 2 + k % 3]

    def picked(h, w):
        return (pg, pu, pd)[w].at[h]

    def hot_at(h, lay, half, w):
        if w == 2:
            return h2.at[lay, h, pl.ds(pl.multiple_of(half * f_loc, 128), f_loc)]
        return h13.at[lay, h, :, cols(half, w)]

    stays = (x == y) & (c == x)

    def home_refs(j, i, b0, w):
        b1, b2 = (z + i) % 2, (c + j) % 2
        src = (wg, wu, wd)[w].at[0, 4 * b2 + 2 * b1 + b0]
        if w == 2 and b0 == 1:
            src = src.at[pl.ds(tail_rows, kept)]
            dst = o2b.at[y, pl.ds(pl.multiple_of(z * kept, 128), kept)]
        elif w == 2:
            dst = o2.at[y, pl.ds(pl.multiple_of(z * f_loc, 128), f_loc)]
        else:
            dst = o13.at[y, b0, :, cols(z, w)]
        return src, dst, rg_recv.at[w, b0, y * 2 + z], (b1, x, c * 2 + b2)

    def home_copy(j, i, b0, w):
        src, dst, recv, dev = home_refs(j, i, b0, w)
        return remote(src, dst, rg_send.at[w, 4 * j + 2 * i + b0], recv, dev)

    def home_start(j, i, b0, w):
        if (j, i) != (0, 0):
            home_copy(j, i, b0, w).start()
            return

        @pl.when(stays)
        def _():
            src, dst, recv, _ = home_refs(j, i, b0, w)
            pltpu.make_async_copy(src, dst, recv).start()

        @pl.when(jnp.logical_not(stays))
        def _():
            home_copy(j, i, b0, w).start()

    def home_sent(j, i, b0, w):
        if (j, i) != (0, 0):
            home_copy(j, i, b0, w).wait_send()
            return

        @pl.when(jnp.logical_not(stays))
        def _():
            home_copy(j, i, b0, w).wait_send()

    homes = [
        (j, i, b0, w)
        for b0 in range(2) for w in range(3) for j in range(2) for i in range(2)
    ]

    tails = []
    for n in range(4):
        e = 4 * ((c + y + n % 2) % 2) + 2 * ((z + n // 2) % 2) + 1
        tails.append((
            pltpu.make_async_copy(wd.at[0, e, pl.ds(0, tail_rows)], held.at[n], t_sem.at[0, n]),
            pltpu.make_async_copy(held.at[n], (t0, t1, t2, t3)[n], t_sem.at[1, n]),
        ))

    CH = range(6)
    dd = [remote(picked(2 * (1 - c) + k // 3, k % 3), vmem(par13, par2, k), dd_send.at[k], dd_recv.at[k], partner) for k in CH]
    own = [pltpu.make_async_copy(picked(2 * c + k // 3, k % 3), vmem(own13, own2, k), loc_sem.at[k]) for k in CH]
    xs = [remote(vmem(own13, own2, k), vmem(far13, far2, k), x_send.at[k], x_recv.at[k], x_nbr) for k in CH]

    def choose(take_a, a, b, out):
        rows = a.shape[0] // 8

        def body(i, carry):
            at = pl.ds(pl.multiple_of(i * rows, 16), rows)
            out[at, :] = jnp.where(take_a, a[at, :], b[at, :])
            return carry

        lax.fori_loop(0, 8, body, 0)

    for k in CH:
        own[k].start()
        dd[k].start()
    for b in homes[:2]:
        home_start(*b)
    for k in CH:
        own[k].wait()
        dd[k].wait_recv()
        owner = owner_ref[2 * c + k // 3]
        choose(owner % 2 == c, vmem(own13, own2, k), vmem(par13, par2, k), vmem(own13, own2, k))
        if k > 0:
            xs[k - 1].start()
    for b in homes[2:4]:
        home_start(*b)
    xs[5].start()

    @pl.when(c != x)
    def _():
        for b in homes[4:]:
            home_start(*b)

    def spread(first, stop):
        @pl.when(c == x)
        def _():
            for b in homes[first:stop]:
                home_start(*b)

    spread(4, 6)

    def hot_of(k):
        return 2 * c + k // 3

    def fan(k):
        src, w = vmem(par13, par2, k), k % 3
        dst = hot_at(hot_of(k), y, z, w)
        return (
            remote(src, dst, n_send.at[0, k], n_recv.at[0, k], y_nbr),
            remote(src, dst, n_send.at[1, k], n_recv.at[1, k], z_nbr),
            remote(src, dst, q_send.at[0, k], q_recv.at[0, k], partner),
            pltpu.make_async_copy(src, dst, w_sem.at[k]),
        )

    def from_y(k):
        at = hot_at(hot_of(k), 1 - y, z, k % 3)
        return at, remote(at, at, q_send.at[1, k], q_recv.at[1, k], partner)

    def from_z(k):
        at = hot_at(hot_of(k), y, 1 - z, k % 3)
        return at, remote(at, at, q_send.at[2, k], q_recv.at[2, k], partner)

    def onward(k):
        if k % 2 == 0:
            at = hot_at(hot_of(k), 1 - y, z, k % 3)
            return remote(at, at, n_send.at[2, k], n_recv.at[2, k], z_nbr)
        at = hot_at(hot_of(k), y, 1 - z, k % 3)
        return remote(at, at, n_send.at[2, k], n_recv.at[2, k], y_nbr)

    def across(k):
        at = hot_at(hot_of(k), 1 - y, 1 - z, k % 3)
        return remote(at, at, f_send.at[k], n_recv.at[2, k], x_nbr)

    def onward_do(k, what):
        if k < 4:
            pl.when(c == x)(lambda: what(onward(k)))
        else:
            what(onward(k))

    def from_diag(k):
        at = hot_at(hot_of(k), 1 - y, 1 - z, k % 3)
        return at, remote(at, at, q_send.at[3, k], q_recv.at[3, k], partner)

    def landed(at, sem):
        pltpu.make_async_copy(at, at, sem).wait()

    for load, _ in tails:
        load.start()
    for load, store in tails:
        load.wait()
        store.start()
    for k in CH:
        xs[k].wait_recv()
        owner = owner_ref[2 * c + k // 3]
        choose(owner // 2 == x, vmem(own13, own2, k), vmem(far13, far2, k), vmem(par13, par2, k))
        if k > 0:
            for copy in fan(k - 1):
                copy.start()
        spread(6 + k, 7 + k)
    for copy in fan(5):
        copy.start()
    spread(12, len(homes))
    for k in CH:
        at, pass_on = from_y(k)
        landed(at, n_recv.at[0, k])
        if k % 2 == 0:
            onward_do(k, lambda copy: copy.start())
        pass_on.start()
        at, pass_on = from_z(k)
        landed(at, n_recv.at[1, k])
        if k % 2 == 1:
            onward_do(k, lambda copy: copy.start())
        pass_on.start()
    for k in CH:
        at, pass_on = from_diag(k)
        landed(at, n_recv.at[2, k])
        if k < 4:
            pl.when(c == x)(lambda: across(k).start())
        pass_on.start()

    for _, store in tails:
        store.wait()
    for k in CH:
        dd[k].wait_send()
        to_y, to_z, to_p, to_self = fan(k)
        to_y.wait_send()
        to_z.wait_send()
        to_p.wait_send()
        to_self.wait()
        xs[k].wait_send()
        onward_do(k, lambda copy: copy.wait_send())
        if k < 4:
            pl.when(c == x)(lambda: across(k).wait_send())
        from_y(k)[1].wait_send()
        from_z(k)[1].wait_send()
        from_diag(k)[1].wait_send()
    for k in CH:
        h, w = 2 * (1 - c) + k // 3, k % 3
        landed(hot_at(h, y, z, w), q_recv.at[0, k])
        landed(hot_at(h, 1 - y, z, w), q_recv.at[1, k])
        landed(hot_at(h, y, 1 - z, w), q_recv.at[2, k])
        landed(hot_at(h, 1 - y, 1 - z, w), q_recv.at[3, k])
    for b in homes:
        home_sent(*b)
    for w in range(3):
        for b0 in range(2):
            for lay in range(2):
                for half in range(2):
                    if w == 2 and b0 == 1:
                        at = o2b.at[lay, pl.ds(half * kept, kept)]
                    elif w == 2:
                        at = o2.at[lay, pl.ds(half * f_loc, f_loc)]
                    else:
                        at = o13.at[lay, b0, :, pl.ds(half * f_loc + w * f_all, f_loc)]
                    landed(at, rg_recv.at[w, b0, lay * 2 + half])


def settle_kernel(o13, o2, o2b, h13, h2, q13, q2, g13, g2, buf13, buf2, sems):
    slots = buf13.shape[0]
    rows13, rows2 = buf13.shape[1], buf2.shape[1]

    def tiles(src, dst, rows, buf):
        return [
            (src.at[pl.ds(r, rows)], dst.at[pl.ds(r, rows)], buf) for r in range(0, src.shape[0], rows)
        ]

    kept = o2b.shape[1] // 2

    work = []
    for lay in range(2):
        for n in range(o13.shape[1]):
            work += tiles(o13.at[lay, n], q13.at[lay, n], rows13, buf13)
        work += tiles(o2.at[lay], q2.at[lay, 0], rows2, buf2)
        for half in range(2):
            put = q2.at[lay, 1, pl.ds((half + 1) * rows2 - kept, kept)]
            work.append((o2b.at[lay, pl.ds(half * kept, kept)], put, buf2))
        for n in range(h13.shape[1]):
            work += tiles(h13.at[lay, n], g13.at[lay, n], rows13, buf13)
            work += tiles(h2.at[lay, n], g2.at[lay, n], rows2, buf2)

    used = {id(buf13): 0, id(buf2): 0}
    steps = []
    last = {}
    for src, dst, buf in work:
        kind = 0 if buf is buf13 else 1
        slot = used[id(buf)] % slots
        used[id(buf)] += 1
        before = last.get((kind, slot))
        tile = buf.at[slot, pl.ds(0, src.shape[0])]
        step = (
            pltpu.make_async_copy(src, tile, sems.at[kind, 0, slot]),
            pltpu.make_async_copy(tile, dst, sems.at[kind, 1, slot]),
            before,
        )
        last[kind, slot] = step
        steps.append(step)
    lag = slots // 2
    for n in range(len(steps) + lag):
        if n < len(steps):
            load, _, before = steps[n]
            if before is not None:
                before[1].wait()
            load.start()
        if n >= lag:
            load, store, _ = steps[n - lag]
            load.wait()
            store.start()
    for step in last.values():
        step[1].wait()


def place_kernel(t0, t1, r0, r1, r2, r3, q2_in, q2, buf, sems):
    z = lax.axis_index("fs")
    y = lax.axis_index("pp")
    ep = lax.axis_index("ep")
    x, c = ep // 2, ep % 2
    f_loc, tail_rows = q2.shape[2] // 2, buf.shape[1]

    def each(n, what):
        source = (r0, r1, r2, r3)[n]
        if n >= 2:
            what(source)
            return
        here = (x == y) & (c == x) & (y == n)
        pl.when(here)(lambda: what((t0, t1)[n]))
        pl.when(jnp.logical_not(here))(lambda: what(source))

    def store(n):
        lay, half = (c + x + n % 2) % 2, (z + n // 2) % 2
        rows = pl.ds(pl.multiple_of(half * f_loc, 128), tail_rows)
        return pltpu.make_async_copy(buf.at[n], q2.at[lay, 1, rows], sems.at[1, n])

    for n in range(4):
        each(n, lambda src: pltpu.make_async_copy(src, buf.at[n], sems.at[0, n]).start())
    for n in range(4):
        pltpu.make_async_copy(r0, buf.at[n], sems.at[0, n]).wait()
        store(n).start()
    for n in range(4):
        store(n).wait()


def solution(mesh):
    fs_size, pp_size, ep_size = mesh.shape["fs"], mesh.shape["pp"], mesh.shape["ep"]
    in_spec = P("pp", "ep", None, "fs")
    down_spec = P("pp", "ep", "fs", None)
    home_spec = P(None, ("pp", "ep", "fs"), None, None)

    def tail_pairs(n):
        pairs = []
        for z in range(fs_size):
            for y in range(pp_size):
                for ep in range(ep_size):
                    x, c = ep // 2, ep % 2
                    b1, b2 = (z + n // 2) % 2, (c + y + n % 2) % 2
                    src = (z * pp_size + y) * ep_size + ep
                    dst = (b1 * pp_size + x) * ep_size + c * 2 + b2
                    if src != dst:
                        pairs.append((src, dst))
        return pairs

    def device_body(w_gate, w_up, w_down, hot_ids):
        dtype = w_gate.dtype
        lay, exp_local, d_model, f_loc = w_gate.shape
        hot = hot_ids.shape[0]
        layers, f_all = lay * pp_size, f_loc * fs_size
        home = exp_local // (fs_size * pp_size)
        offset = jnp.clip(hot_ids - lax.axis_index("ep") * exp_local, 0, exp_local - 1)
        owner = hot_ids // exp_local
        picked = pick_hot(w_gate, w_up, w_down, offset)
        dma = pltpu.SemaphoreType.DMA
        buf13 = pltpu.VMEM((4, d_model, f_loc), dtype)
        buf2 = pltpu.VMEM((2, f_loc, d_model), dtype)
        shape = lambda *dims: jax.ShapeDtypeStruct(dims, dtype)
        tail_rows = f_loc * 2 // 3
        held = pltpu.VMEM((4, tail_rows, d_model), dtype)
        o13, o2, o2b, h13, h2, *tail = pl.pallas_call(
            move_kernel,
            out_shape=[
                shape(layers, home, d_model, 2 * f_all),
                shape(layers, f_all, d_model),
                shape(layers, f_all - fs_size * tail_rows, d_model),
                shape(layers, hot, d_model, 2 * f_all),
                shape(layers, hot, f_all, d_model),
            ] + [shape(tail_rows, d_model)] * 4,
            in_specs=[pl.BlockSpec(memory_space=pltpu.SMEM)] + [ANY] * 6,
            out_specs=[ANY] * 9,
            scratch_shapes=[
                buf13, buf2, buf13, buf2, buf13, buf2, held, dma((2, 4)),
                dma((3, 8)), dma((3, 2, 4)), dma((6,)), dma((6,)), dma((6,)), dma((6,)), dma((6,)),
                dma((3, 6)), dma((3, 6)), dma((4,)), dma((4, 6)), dma((4, 6)), dma((6,)),
            ],
            compiler_params=pltpu.CompilerParams(has_side_effects=True, vmem_limit_bytes=48 * 1024 * 1024),
        )(owner, w_gate, w_up, w_down, *picked)
        moved = [lax.ppermute(t, ("fs", "pp", "ep"), tail_pairs(n)) for n, t in enumerate(tail)]
        copied = 4 * (o13.size + o2.size + h13.size + h2.size)
        q13, q2, g13, g2 = pl.pallas_call(
            settle_kernel,
            out_shape=[
                shape(*o13.shape), shape(layers, home, f_all, d_model), shape(*h13.shape), shape(*h2.shape),
            ],
            in_specs=[ANY] * 5,
            out_specs=[ANY] * 4,
            scratch_shapes=[
                pltpu.VMEM((12, 512, 2 * f_all), dtype), pltpu.VMEM((12, f_loc, d_model), dtype), dma((2, 2, 12)),
            ],
            cost_estimate=pl.CostEstimate(flops=10**9, bytes_accessed=copied, transcendentals=0),
            compiler_params=pltpu.CompilerParams(vmem_limit_bytes=48 * 1024 * 1024),
        )(o13, o2, o2b, h13, h2)
        q2 = pl.pallas_call(
            place_kernel,
            out_shape=shape(*q2.shape),
            in_specs=[ANY] * 7,
            out_specs=ANY,
            scratch_shapes=[held, dma((2, 4))],
            input_output_aliases={6: 0},
            compiler_params=pltpu.CompilerParams(vmem_limit_bytes=56 * 1024 * 1024),
        )(tail[0], tail[1], *moved, q2)
        return q13, q2, g13, g2

    return jax.shard_map(
        device_body,
        mesh=mesh,
        in_specs=(in_spec, in_spec, down_spec, P()),
        out_specs=(home_spec, home_spec, P(), P()),
        check_vma=False,
    )
```

```python
import functools

import jax
import jax.numpy as jnp
from jax import lax
from jax.experimental import pallas as pl
from jax.experimental.pallas import tpu as pltpu
from jax.sharding import PartitionSpec as P

MESH = pl.DeviceIdType.MESH
ANY = pl.BlockSpec(memory_space=pl.ANY)


def pick_kernel(off_ref, g_ref, u_ref, d_ref, pg_ref, pu_ref, pd_ref):
    pg_ref[...] = g_ref[0]
    pu_ref[...] = u_ref[0]
    pd_ref[...] = d_ref[0]


def pick_hot(w_gate, w_up, w_down, offset):
    hot = offset.shape[0]
    _, _, d_model, f_loc = w_gate.shape
    take_in = lambda h, off: (0, off[h], 0, 0)
    put = lambda h, off: (h, 0, 0)
    shape_in = jax.ShapeDtypeStruct((hot, d_model, f_loc), w_gate.dtype)
    shape_down = jax.ShapeDtypeStruct((hot, f_loc, d_model), w_gate.dtype)
    return pl.pallas_call(
        pick_kernel,
        grid_spec=pltpu.PrefetchScalarGridSpec(
            num_scalar_prefetch=1,
            grid=(hot,),
            in_specs=[
                pl.BlockSpec((1, 1, d_model, f_loc), take_in),
                pl.BlockSpec((1, 1, d_model, f_loc), take_in),
                pl.BlockSpec((1, 1, f_loc, d_model), take_in),
            ],
            out_specs=[
                pl.BlockSpec((1, d_model, f_loc), put),
                pl.BlockSpec((1, d_model, f_loc), put),
                pl.BlockSpec((1, f_loc, d_model), put),
            ],
        ),
        out_shape=[shape_in, shape_in, shape_down],
    )(offset, w_gate, w_up, w_down)


def place_of_device():
    z = lax.axis_index("fs")
    y = lax.axis_index("pp")
    ep = lax.axis_index("ep")
    return ep // 2, y, z, ep % 2


def remote(src, dst, send, recv, dev):
    return pltpu.make_async_remote_copy(
        src_ref=src, dst_ref=dst, send_sem=send, recv_sem=recv, device_id=dev, device_id_type=MESH
    )


def landed(at, sem):
    pltpu.make_async_copy(at, at, sem).wait()


def home_kernel(wg, wu, wd, o13, o2, o2b, t0, t1, t2, t3, held, t_sem, rg_send, rg_recv):
    x, y, z, c = place_of_device()
    f_loc = wg.shape[3]
    f_all = f_loc * 2
    tail_rows = t0.shape[0]
    kept = f_loc - tail_rows

    stays = (x == y) & (c == x)

    def home_refs(j, i, b0, w):
        b1, b2 = (z + i) % 2, (c + j) % 2
        src = (wg, wu, wd)[w].at[0, 4 * b2 + 2 * b1 + b0]
        if w == 2 and b0 == 1:
            src = src.at[pl.ds(tail_rows, kept)]
            dst = o2b.at[y, pl.ds(pl.multiple_of(z * kept, 128), kept)]
        elif w == 2:
            dst = o2.at[y, pl.ds(pl.multiple_of(z * f_loc, 128), f_loc)]
        else:
            dst = o13.at[y, b0, :, pl.ds(pl.multiple_of(z * f_loc + w * f_all, 128), f_loc)]
        return src, dst, rg_recv.at[w, b0, y * 2 + z], (b1, x, c * 2 + b2)

    def home_copy(j, i, b0, w):
        src, dst, recv, dev = home_refs(j, i, b0, w)
        return remote(src, dst, rg_send.at[w, 4 * j + 2 * i + b0], recv, dev)

    def home_start(j, i, b0, w):
        if (j, i) != (0, 0):
            home_copy(j, i, b0, w).start()
            return

        @pl.when(stays)
        def _():
            src, dst, recv, _ = home_refs(j, i, b0, w)
            pltpu.make_async_copy(src, dst, recv).start()

        @pl.when(jnp.logical_not(stays))
        def _():
            home_copy(j, i, b0, w).start()

    def home_sent(j, i, b0, w):
        if (j, i) != (0, 0):
            home_copy(j, i, b0, w).wait_send()
            return

        @pl.when(jnp.logical_not(stays))
        def _():
            home_copy(j, i, b0, w).wait_send()

    homes = [(j, i, b0, w) for b0 in range(2) for w in range(3) for j in range(2) for i in range(2)]

    tails = []
    for n in range(4):
        e = 4 * ((c + y + n % 2) % 2) + 2 * ((z + n // 2) % 2) + 1
        tails.append((
            pltpu.make_async_copy(wd.at[0, e, pl.ds(0, tail_rows)], held.at[n], t_sem.at[0, n]),
            pltpu.make_async_copy(held.at[n], (t0, t1, t2, t3)[n], t_sem.at[1, n]),
        ))

    for b in homes:
        home_start(*b)
    for load, _ in tails:
        load.start()
    for load, store in tails:
        load.wait()
        store.start()
    for _, store in tails:
        store.wait()
    for b in homes:
        home_sent(*b)
    for w in range(3):
        for b0 in range(2):
            for lay in range(2):
                for half in range(2):
                    if w == 2 and b0 == 1:
                        at = o2b.at[lay, pl.ds(half * kept, kept)]
                    elif w == 2:
                        at = o2.at[lay, pl.ds(half * f_loc, f_loc)]
                    else:
                        at = o13.at[lay, b0, :, pl.ds(half * f_loc + w * f_all, f_loc)]
                    landed(at, rg_recv.at[w, b0, lay * 2 + half])


def hot_kernel(
    owner_ref, pg, pu, pd, h13, h2,
    own13, own2, par13, par2, far13, far2,
    loc_sem, dd_send, dd_recv, x_send, x_recv, n_send, n_recv, q_send, q_recv, w_sem,
):
    x, y, z, c = place_of_device()
    f_loc = pg.shape[2]
    f_all = f_loc * 2
    partner = (z, y, x * 2 + 1 - c)
    x_nbr = (z, y, (1 - x) * 2 + c)
    y_nbr = (z, 1 - y, x * 2 + c)
    z_nbr = (1 - z, y, x * 2 + c)

    def vmem(b13, b2, k):
        return b2.at[k // 3] if k % 3 == 2 else b13.at[(k // 3) * 2 + k % 3]

    def picked(h, w):
        return (pg, pu, pd)[w].at[h]

    def hot_at(h, lay, half, w):
        if w == 2:
            return h2.at[lay, h, pl.ds(pl.multiple_of(half * f_loc, 128), f_loc)]
        return h13.at[lay, h, :, pl.ds(pl.multiple_of(half * f_loc + w * f_all, 128), f_loc)]

    CH = range(6)
    dd = [remote(picked(2 * (1 - c) + k // 3, k % 3), vmem(par13, par2, k), dd_send.at[k], dd_recv.at[k], partner) for k in CH]
    own = [pltpu.make_async_copy(picked(2 * c + k // 3, k % 3), vmem(own13, own2, k), loc_sem.at[k]) for k in CH]
    xs = [remote(vmem(own13, own2, k), vmem(far13, far2, k), x_send.at[k], x_recv.at[k], x_nbr) for k in CH]

    def choose(take_a, a, b, out):
        rows = a.shape[0] // 8

        def body(i, carry):
            at = pl.ds(pl.multiple_of(i * rows, 16), rows)
            out[at, :] = jnp.where(take_a, a[at, :], b[at, :])
            return carry

        lax.fori_loop(0, 8, body, 0)

    def hot_of(k):
        return 2 * c + k // 3

    def fan(k):
        src, w = vmem(par13, par2, k), k % 3
        dst = hot_at(hot_of(k), y, z, w)
        return (
            remote(src, dst, n_send.at[0, k], n_recv.at[0, k], y_nbr),
            remote(src, dst, n_send.at[1, k], n_recv.at[1, k], z_nbr),
            remote(src, dst, q_send.at[0, k], q_recv.at[0, k], partner),
            pltpu.make_async_copy(src, dst, w_sem.at[k]),
        )

    def from_y(k):
        at = hot_at(hot_of(k), 1 - y, z, k % 3)
        return at, remote(at, at, q_send.at[1, k], q_recv.at[1, k], partner)

    def from_z(k):
        at = hot_at(hot_of(k), y, 1 - z, k % 3)
        return at, remote(at, at, q_send.at[2, k], q_recv.at[2, k], partner)

    def onward(k):
        if k % 2 == 0:
            at = hot_at(hot_of(k), 1 - y, z, k % 3)
            return remote(at, at, n_send.at[2, k], n_recv.at[2, k], z_nbr)
        at = hot_at(hot_of(k), y, 1 - z, k % 3)
        return remote(at, at, n_send.at[2, k], n_recv.at[2, k], y_nbr)

    def from_diag(k):
        at = hot_at(hot_of(k), 1 - y, 1 - z, k % 3)
        return at, remote(at, at, q_send.at[3, k], q_recv.at[3, k], partner)

    for k in CH:
        own[k].start()
        dd[k].start()
    for s in range(11):
        if s < 6:
            own[s].wait()
            dd[s].wait_recv()
            owner = owner_ref[2 * c + s // 3]
            choose(owner % 2 == c, vmem(own13, own2, s), vmem(par13, par2, s), vmem(own13, own2, s))
        if 1 <= s <= 6:
            xs[s - 1].start()
        k = s - 3
        if 0 <= k < 6:
            xs[k].wait_recv()
            owner = owner_ref[2 * c + k // 3]
            choose(owner // 2 == x, vmem(own13, own2, k), vmem(far13, far2, k), vmem(par13, par2, k))
        k = s - 4
        if 0 <= k < 6:
            for copy in fan(k):
                copy.start()
    for k in CH:
        at, pass_on = from_y(k)
        landed(at, n_recv.at[0, k])
        if k % 2 == 0:
            onward(k).start()
        pass_on.start()
        at, pass_on = from_z(k)
        landed(at, n_recv.at[1, k])
        if k % 2 == 1:
            onward(k).start()
        pass_on.start()
    for k in CH:
        at, pass_on = from_diag(k)
        landed(at, n_recv.at[2, k])
        pass_on.start()

    for k in CH:
        dd[k].wait_send()
        xs[k].wait_send()
        to_y, to_z, to_p, to_self = fan(k)
        to_y.wait_send()
        to_z.wait_send()
        to_p.wait_send()
        to_self.wait()
        onward(k).wait_send()
        from_y(k)[1].wait_send()
        from_z(k)[1].wait_send()
        from_diag(k)[1].wait_send()
    for k in CH:
        h, w = 2 * (1 - c) + k // 3, k % 3
        landed(hot_at(h, y, z, w), q_recv.at[0, k])
        landed(hot_at(h, 1 - y, z, w), q_recv.at[1, k])
        landed(hot_at(h, y, 1 - z, w), q_recv.at[2, k])
        landed(hot_at(h, 1 - y, 1 - z, w), q_recv.at[3, k])


def settle_kernel(o13, o2, o2b, h13, h2, q13, q2, g13, g2, buf13, buf2, sems):
    slots = buf13.shape[0]
    rows13, rows2 = buf13.shape[1], buf2.shape[1]

    def tiles(src, dst, rows, buf):
        return [
            (src.at[pl.ds(r, rows)], dst.at[pl.ds(r, rows)], buf) for r in range(0, src.shape[0], rows)
        ]

    kept = o2b.shape[1] // 2

    work = []
    for lay in range(2):
        for n in range(o13.shape[1]):
            work += tiles(o13.at[lay, n], q13.at[lay, n], rows13, buf13)
        work += tiles(o2.at[lay], q2.at[lay, 0], rows2, buf2)
        for half in range(2):
            put = q2.at[lay, 1, pl.ds((half + 1) * rows2 - kept, kept)]
            work.append((o2b.at[lay, pl.ds(half * kept, kept)], put, buf2))
        for n in range(h13.shape[1]):
            work += tiles(h13.at[lay, n], g13.at[lay, n], rows13, buf13)
            work += tiles(h2.at[lay, n], g2.at[lay, n], rows2, buf2)

    used = {id(buf13): 0, id(buf2): 0}
    steps = []
    last = {}
    for src, dst, buf in work:
        kind = 0 if buf is buf13 else 1
        slot = used[id(buf)] % slots
        used[id(buf)] += 1
        before = last.get((kind, slot))
        tile = buf.at[slot, pl.ds(0, src.shape[0])]
        step = (
            pltpu.make_async_copy(src, tile, sems.at[kind, 0, slot]),
            pltpu.make_async_copy(tile, dst, sems.at[kind, 1, slot]),
            before,
        )
        last[kind, slot] = step
        steps.append(step)
    lag = slots // 2
    for n in range(len(steps) + lag):
        if n < len(steps):
            load, _, before = steps[n]
            if before is not None:
                before[1].wait()
            load.start()
        if n >= lag:
            load, store, _ = steps[n - lag]
            load.wait()
            store.start()
    for step in last.values():
        step[1].wait()


def place_kernel(t0, t1, r0, r1, r2, r3, q2_in, q2, buf, sems):
    z = lax.axis_index("fs")
    y = lax.axis_index("pp")
    ep = lax.axis_index("ep")
    x, c = ep // 2, ep % 2
    f_loc, tail_rows = q2.shape[2] // 2, buf.shape[1]

    def each(n, what):
        source = (r0, r1, r2, r3)[n]
        if n >= 2:
            what(source)
            return
        here = (x == y) & (c == x) & (y == n)
        pl.when(here)(lambda: what((t0, t1)[n]))
        pl.when(jnp.logical_not(here))(lambda: what(source))

    def store(n):
        lay, half = (c + x + n % 2) % 2, (z + n // 2) % 2
        rows = pl.ds(pl.multiple_of(half * f_loc, 128), tail_rows)
        return pltpu.make_async_copy(buf.at[n], q2.at[lay, 1, rows], sems.at[1, n])

    for n in range(4):
        each(n, lambda src: pltpu.make_async_copy(src, buf.at[n], sems.at[0, n]).start())
    for n in range(4):
        pltpu.make_async_copy(r0, buf.at[n], sems.at[0, n]).wait()
        store(n).start()
    for n in range(4):
        store(n).wait()


def solution(mesh):
    fs_size, pp_size, ep_size = mesh.shape["fs"], mesh.shape["pp"], mesh.shape["ep"]
    in_spec = P("pp", "ep", None, "fs")
    down_spec = P("pp", "ep", "fs", None)
    home_spec = P(None, ("pp", "ep", "fs"), None, None)

    def tail_pairs(n):
        pairs = []
        for z in range(fs_size):
            for y in range(pp_size):
                for ep in range(ep_size):
                    x, c = ep // 2, ep % 2
                    b1, b2 = (z + n // 2) % 2, (c + y + n % 2) % 2
                    src = (z * pp_size + y) * ep_size + ep
                    dst = (b1 * pp_size + x) * ep_size + c * 2 + b2
                    if src != dst:
                        pairs.append((src, dst))
        return pairs

    def device_body(w_gate, w_up, w_down, hot_ids):
        dtype = w_gate.dtype
        lay, exp_local, d_model, f_loc = w_gate.shape
        hot = hot_ids.shape[0]
        layers, f_all = lay * pp_size, f_loc * fs_size
        home = exp_local // (fs_size * pp_size)
        offset = jnp.clip(hot_ids - lax.axis_index("ep") * exp_local, 0, exp_local - 1)
        owner = hot_ids // exp_local
        picked = pick_hot(w_gate, w_up, w_down, offset)
        dma = pltpu.SemaphoreType.DMA
        buf13 = pltpu.VMEM((4, d_model, f_loc), dtype)
        buf2 = pltpu.VMEM((2, f_loc, d_model), dtype)
        shape = lambda *dims: jax.ShapeDtypeStruct(dims, dtype)
        tail_rows = f_loc * 2 // 3
        held = pltpu.VMEM((4, tail_rows, d_model), dtype)
        h13, h2 = pl.pallas_call(
            hot_kernel,
            out_shape=[
                shape(layers, hot, d_model, 2 * f_all),
                shape(layers, hot, f_all, d_model),
            ],
            in_specs=[pl.BlockSpec(memory_space=pltpu.SMEM)] + [ANY] * 3,
            out_specs=[ANY] * 2,
            scratch_shapes=[
                buf13, buf2, buf13, buf2, buf13, buf2,
                dma((6,)), dma((6,)), dma((6,)), dma((6,)), dma((6,)),
                dma((3, 6)), dma((3, 6)), dma((4, 6)), dma((4, 6)), dma((6,)),
            ],
            compiler_params=pltpu.CompilerParams(has_side_effects=True, vmem_limit_bytes=48 * 1024 * 1024),
        )(owner, *picked)
        o13, o2, o2b, *tail = pl.pallas_call(
            home_kernel,
            out_shape=[
                shape(layers, home, d_model, 2 * f_all),
                shape(layers, f_all, d_model),
                shape(layers, f_all - fs_size * tail_rows, d_model),
            ] + [shape(tail_rows, d_model)] * 4,
            in_specs=[ANY] * 3,
            out_specs=[ANY] * 7,
            scratch_shapes=[held, dma((2, 4)), dma((3, 8)), dma((3, 2, 4))],
            compiler_params=pltpu.CompilerParams(has_side_effects=True, vmem_limit_bytes=48 * 1024 * 1024),
        )(w_gate, w_up, w_down)
        moved = [lax.ppermute(t, ("fs", "pp", "ep"), tail_pairs(n)) for n, t in enumerate(tail)]
        copied = 4 * (o13.size + o2.size + h13.size + h2.size)
        q13, q2, g13, g2 = pl.pallas_call(
            settle_kernel,
            out_shape=[
                shape(*o13.shape), shape(layers, home, f_all, d_model), shape(*h13.shape), shape(*h2.shape),
            ],
            in_specs=[ANY] * 5,
            out_specs=[ANY] * 4,
            scratch_shapes=[
                pltpu.VMEM((12, 512, 2 * f_all), dtype), pltpu.VMEM((12, f_loc, d_model), dtype), dma((2, 2, 12)),
            ],
            cost_estimate=pl.CostEstimate(flops=10**9, bytes_accessed=copied, transcendentals=0),
            compiler_params=pltpu.CompilerParams(vmem_limit_bytes=48 * 1024 * 1024),
        )(o13, o2, o2b, h13, h2)
        q2 = pl.pallas_call(
            place_kernel,
            out_shape=shape(*q2.shape),
            in_specs=[ANY] * 7,
            out_specs=ANY,
            scratch_shapes=[held, dma((2, 4))],
            input_output_aliases={6: 0},
            compiler_params=pltpu.CompilerParams(vmem_limit_bytes=56 * 1024 * 1024),
        )(tail[0], tail[1], *moved, q2)
        return q13, q2, g13, g2

    return jax.shard_map(
        device_body,
        mesh=mesh,
        in_specs=(in_spec, in_spec, down_spec, P()),
        out_specs=(home_spec, home_spec, P(), P()),
        check_vma=False,
    )
```

```python
import functools

import jax
import jax.numpy as jnp
from jax import lax
from jax.experimental import pallas as pl
from jax.experimental.pallas import tpu as pltpu
from jax.sharding import PartitionSpec as P

MESH = pl.DeviceIdType.MESH
ANY = pl.BlockSpec(memory_space=pl.ANY)


def pick_kernel(off_ref, g_ref, u_ref, d_ref, pg_ref, pu_ref, pd_ref):
    pg_ref[...] = g_ref[0]
    pu_ref[...] = u_ref[0]
    pd_ref[...] = d_ref[0]


def pick_hot(w_gate, w_up, w_down, offset):
    hot = offset.shape[0]
    _, _, d_model, f_loc = w_gate.shape
    take_in = lambda h, off: (0, off[h], 0, 0)
    put = lambda h, off: (h, 0, 0)
    shape_in = jax.ShapeDtypeStruct((hot, d_model, f_loc), w_gate.dtype)
    shape_down = jax.ShapeDtypeStruct((hot, f_loc, d_model), w_gate.dtype)
    return pl.pallas_call(
        pick_kernel,
        grid_spec=pltpu.PrefetchScalarGridSpec(
            num_scalar_prefetch=1,
            grid=(hot,),
            in_specs=[
                pl.BlockSpec((1, 1, d_model, f_loc), take_in),
                pl.BlockSpec((1, 1, d_model, f_loc), take_in),
                pl.BlockSpec((1, 1, f_loc, d_model), take_in),
            ],
            out_specs=[
                pl.BlockSpec((1, d_model, f_loc), put),
                pl.BlockSpec((1, d_model, f_loc), put),
                pl.BlockSpec((1, f_loc, d_model), put),
            ],
        ),
        out_shape=[shape_in, shape_in, shape_down],
    )(offset, w_gate, w_up, w_down)


def move_kernel(
    owner_ref, wg, wu, wd, pg, pu, pd, o13, o2, o2b, h13, h2, t0, t1, t2, t3,
    own13, own2, par13, par2, far13, far2, held, t_sem,
    rg_send, rg_recv, loc_sem, dd_send, dd_recv, x_send, x_recv,
    n_send, n_recv, f_send, q_send, q_recv, w_sem,
):
    z = lax.axis_index("fs")
    y = lax.axis_index("pp")
    ep = lax.axis_index("ep")
    x, c = ep // 2, ep % 2
    d_model, f_loc = wg.shape[2], wg.shape[3]
    f_all = f_loc * 2
    tail_rows = t0.shape[0]
    kept = f_loc - tail_rows
    partner = (z, y, x * 2 + 1 - c)
    x_nbr = (z, y, (1 - x) * 2 + c)
    y_nbr = (z, 1 - y, ep)
    z_nbr = (1 - z, y, ep)

    def cols(half, up):
        return pl.ds(pl.multiple_of(half * f_loc + up * f_all, 128), f_loc)

    def remote(src, dst, send, recv, dev):
        return pltpu.make_async_remote_copy(
            src_ref=src, dst_ref=dst, send_sem=send, recv_sem=recv, device_id=dev, device_id_type=MESH
        )

    def vmem(b13, b2, k):
        return b2.at[k // 3] if k % 3 == 2 else b13.at[(k // 3) * 2 + k % 3]

    def picked(h, w):
        return (pg, pu, pd)[w].at[h]

    def hot_at(h, lay, half, w):
        if w == 2:
            return h2.at[lay, h, pl.ds(pl.multiple_of(half * f_loc, 128), f_loc)]
        return h13.at[lay, h, :, cols(half, w)]

    stays = (x == y) & (c == x)

    def home_refs(j, n, b0, w):
        b1, b2 = (z + n + 1 + x + y) % 2, (c + j) % 2
        src = (wg, wu, wd)[w].at[0, 4 * b2 + 2 * b1 + b0]
        if w == 2 and b0 == 1:
            src = src.at[pl.ds(tail_rows, kept)]
            dst = o2b.at[y, pl.ds(pl.multiple_of(z * kept, 128), kept)]
        elif w == 2:
            dst = o2.at[y, pl.ds(pl.multiple_of(z * f_loc, 128), f_loc)]
        else:
            dst = o13.at[y, b0, :, cols(z, w)]
        return src, dst, rg_recv.at[w, b0, y * 2 + z], (b1, x, c * 2 + b2)

    def home_copy(j, n, b0, w):
        src, dst, recv, dev = home_refs(j, n, b0, w)
        return remote(src, dst, rg_send.at[w, 4 * j + 2 * n + b0], recv, dev)

    def home_start(j, n, b0, w):
        if (j, n) != (0, 1):
            home_copy(j, n, b0, w).start()
            return

        @pl.when(stays)
        def _():
            src, dst, recv, _ = home_refs(j, n, b0, w)
            pltpu.make_async_copy(src, dst, recv).start()

        @pl.when(jnp.logical_not(stays))
        def _():
            home_copy(j, n, b0, w).start()

    def home_sent(j, n, b0, w):
        if (j, n) != (0, 1):
            home_copy(j, n, b0, w).wait_send()
            return

        @pl.when(jnp.logical_not(stays))
        def _():
            home_copy(j, n, b0, w).wait_send()

    homes = [
        (j, n, b0, w)
        for n in range(2) for b0 in range(2) for w in range(3) for j in range(2)
    ]

    tails = []
    for n in range(4):
        e = 4 * ((c + y + n % 2) % 2) + 2 * ((z + n // 2) % 2) + 1
        tails.append((
            pltpu.make_async_copy(wd.at[0, e, pl.ds(0, tail_rows)], held.at[n], t_sem.at[0, n]),
            pltpu.make_async_copy(held.at[n], (t0, t1, t2, t3)[n], t_sem.at[1, n]),
        ))

    CH = range(6)
    dd = [remote(picked(2 * (1 - c) + k // 3, k % 3), vmem(par13, par2, k), dd_send.at[k], dd_recv.at[k], partner) for k in CH]
    own = [pltpu.make_async_copy(picked(2 * c + k // 3, k % 3), vmem(own13, own2, k), loc_sem.at[k]) for k in CH]
    xs = [remote(vmem(own13, own2, k), vmem(far13, far2, k), x_send.at[k], x_recv.at[k], x_nbr) for k in CH]

    def choose(take_a, a, b, out):
        rows = a.shape[0] // 8

        def body(i, carry):
            at = pl.ds(pl.multiple_of(i * rows, 16), rows)
            out[at, :] = jnp.where(take_a, a[at, :], b[at, :])
            return carry

        lax.fori_loop(0, 8, body, 0)

    for k in CH:
        own[k].start()
        dd[k].start()
    for b in homes[:4]:
        home_start(*b)
    for k in CH:
        own[k].wait()
        dd[k].wait_recv()
        owner = owner_ref[2 * c + k // 3]
        choose(owner % 2 == c, vmem(own13, own2, k), vmem(par13, par2, k), vmem(own13, own2, k))
        if k > 0:
            xs[k - 1].start()
    for load, _ in tails:
        load.start()
    xs[5].start()

    @pl.when(c != x)
    def _():
        for b in homes[4:]:
            home_start(*b)

    def spread(first, stop):
        @pl.when(c == x)
        def _():
            for b in homes[first:stop]:
                home_start(*b)

    spread(4, 6)

    def hot_of(k):
        return 2 * c + k // 3

    def fan(k):
        src, w = vmem(par13, par2, k), k % 3
        dst = hot_at(hot_of(k), y, z, w)
        return (
            remote(src, dst, n_send.at[0, k], n_recv.at[0, k], y_nbr),
            remote(src, dst, n_send.at[1, k], n_recv.at[1, k], z_nbr),
            remote(src, dst, q_send.at[0, k], q_recv.at[0, k], partner),
            pltpu.make_async_copy(src, dst, w_sem.at[k]),
        )

    def from_y(k):
        at = hot_at(hot_of(k), 1 - y, z, k % 3)
        return at, remote(at, at, q_send.at[1, k], q_recv.at[1, k], partner)

    def from_z(k):
        at = hot_at(hot_of(k), y, 1 - z, k % 3)
        return at, remote(at, at, q_send.at[2, k], q_recv.at[2, k], partner)

    def onward(k):
        if k % 2 == 0:
            at = hot_at(hot_of(k), 1 - y, z, k % 3)
            return remote(at, at, n_send.at[2, k], n_recv.at[2, k], z_nbr)
        at = hot_at(hot_of(k), y, 1 - z, k % 3)
        return remote(at, at, n_send.at[2, k], n_recv.at[2, k], y_nbr)

    def across(k):
        at = hot_at(hot_of(k), 1 - y, 1 - z, k % 3)
        return remote(at, at, f_send.at[k], n_recv.at[2, k], x_nbr)

    def onward_do(k, what):
        if k < 2:
            pl.when(c == x)(lambda: what(onward(k)))
        else:
            what(onward(k))

    def from_diag(k):
        at = hot_at(hot_of(k), 1 - y, 1 - z, k % 3)
        return at, remote(at, at, q_send.at[3, k], q_recv.at[3, k], partner)

    def landed(at, sem):
        pltpu.make_async_copy(at, at, sem).wait()

    for load, store in tails:
        load.wait()
        store.start()
    for k in CH:
        xs[k].wait_recv()
        owner = owner_ref[2 * c + k // 3]
        choose(owner // 2 == x, vmem(own13, own2, k), vmem(far13, far2, k), vmem(par13, par2, k))
        if k > 0:
            for copy in fan(k - 1):
                copy.start()
    for copy in fan(5):
        copy.start()
    spread(6, 8)
    for k in CH:
        at, pass_on = from_y(k)
        landed(at, n_recv.at[0, k])
        if k % 2 == 0:
            onward_do(k, lambda copy: copy.start())
        pass_on.start()
        at, pass_on = from_z(k)
        landed(at, n_recv.at[1, k])
        if k % 2 == 1:
            onward_do(k, lambda copy: copy.start())
        pass_on.start()
        spread(8 + k, 9 + k)
    spread(14, len(homes))
    for k in CH:
        at, pass_on = from_diag(k)
        landed(at, n_recv.at[2, k])
        if k < 2:
            pl.when(c == x)(lambda: across(k).start())
        pass_on.start()

    for _, store in tails:
        store.wait()
    for k in CH:
        dd[k].wait_send()
        to_y, to_z, to_p, to_self = fan(k)
        to_y.wait_send()
        to_z.wait_send()
        to_p.wait_send()
        to_self.wait()
        xs[k].wait_send()
        onward_do(k, lambda copy: copy.wait_send())
        if k < 2:
            pl.when(c == x)(lambda: across(k).wait_send())
        from_y(k)[1].wait_send()
        from_z(k)[1].wait_send()
        from_diag(k)[1].wait_send()
    for k in CH:
        h, w = 2 * (1 - c) + k // 3, k % 3
        landed(hot_at(h, y, z, w), q_recv.at[0, k])
        landed(hot_at(h, 1 - y, z, w), q_recv.at[1, k])
        landed(hot_at(h, y, 1 - z, w), q_recv.at[2, k])
        landed(hot_at(h, 1 - y, 1 - z, w), q_recv.at[3, k])
    for b in homes:
        home_sent(*b)
    for w in range(3):
        for b0 in range(2):
            for lay in range(2):
                for half in range(2):
                    if w == 2 and b0 == 1:
                        at = o2b.at[lay, pl.ds(half * kept, kept)]
                    elif w == 2:
                        at = o2.at[lay, pl.ds(half * f_loc, f_loc)]
                    else:
                        at = o13.at[lay, b0, :, pl.ds(half * f_loc + w * f_all, f_loc)]
                    landed(at, rg_recv.at[w, b0, lay * 2 + half])


def settle_kernel(o13, o2, o2b, h13, h2, q13, q2, g13, g2, buf13, buf2, sems):
    slots = buf13.shape[0]
    rows13, rows2 = buf13.shape[1], buf2.shape[1]

    def tiles(src, dst, rows, buf):
        return [
            (src.at[pl.ds(r, rows)], dst.at[pl.ds(r, rows)], buf) for r in range(0, src.shape[0], rows)
        ]

    kept = o2b.shape[1] // 2

    work = []
    for lay in range(2):
        for n in range(o13.shape[1]):
            work += tiles(o13.at[lay, n], q13.at[lay, n], rows13, buf13)
        work += tiles(o2.at[lay], q2.at[lay, 0], rows2, buf2)
        for half in range(2):
            put = q2.at[lay, 1, pl.ds((half + 1) * rows2 - kept, kept)]
            work.append((o2b.at[lay, pl.ds(half * kept, kept)], put, buf2))
        for n in range(h13.shape[1]):
            work += tiles(h13.at[lay, n], g13.at[lay, n], rows13, buf13)
            work += tiles(h2.at[lay, n], g2.at[lay, n], rows2, buf2)

    used = {id(buf13): 0, id(buf2): 0}
    steps = []
    last = {}
    for src, dst, buf in work:
        kind = 0 if buf is buf13 else 1
        slot = used[id(buf)] % slots
        used[id(buf)] += 1
        before = last.get((kind, slot))
        tile = buf.at[slot, pl.ds(0, src.shape[0])]
        step = (
            pltpu.make_async_copy(src, tile, sems.at[kind, 0, slot]),
            pltpu.make_async_copy(tile, dst, sems.at[kind, 1, slot]),
            before,
        )
        last[kind, slot] = step
        steps.append(step)
    lag = slots // 2
    for n in range(len(steps) + lag):
        if n < len(steps):
            load, _, before = steps[n]
            if before is not None:
                before[1].wait()
            load.start()
        if n >= lag:
            load, store, _ = steps[n - lag]
            load.wait()
            store.start()
    for step in last.values():
        step[1].wait()


def place_kernel(t0, t1, r0, r1, r2, r3, q2_in, q2, buf, sems):
    z = lax.axis_index("fs")
    y = lax.axis_index("pp")
    ep = lax.axis_index("ep")
    x, c = ep // 2, ep % 2
    f_loc, tail_rows = q2.shape[2] // 2, buf.shape[1]

    def each(n, what):
        source = (r0, r1, r2, r3)[n]
        if n >= 2:
            what(source)
            return
        here = (x == y) & (c == x) & (y == n)
        pl.when(here)(lambda: what((t0, t1)[n]))
        pl.when(jnp.logical_not(here))(lambda: what(source))

    def store(n):
        lay, half = (c + x + n % 2) % 2, (z + n // 2) % 2
        rows = pl.ds(pl.multiple_of(half * f_loc, 128), tail_rows)
        return pltpu.make_async_copy(buf.at[n], q2.at[lay, 1, rows], sems.at[1, n])

    for n in range(4):
        each(n, lambda src: pltpu.make_async_copy(src, buf.at[n], sems.at[0, n]).start())
    for n in range(4):
        pltpu.make_async_copy(r0, buf.at[n], sems.at[0, n]).wait()
        store(n).start()
    for n in range(4):
        store(n).wait()


def solution(mesh):
    fs_size, pp_size, ep_size = mesh.shape["fs"], mesh.shape["pp"], mesh.shape["ep"]
    in_spec = P("pp", "ep", None, "fs")
    down_spec = P("pp", "ep", "fs", None)
    home_spec = P(None, ("pp", "ep", "fs"), None, None)

    def tail_pairs(n):
        pairs = []
        for z in range(fs_size):
            for y in range(pp_size):
                for ep in range(ep_size):
                    x, c = ep // 2, ep % 2
                    b1, b2 = (z + n // 2) % 2, (c + y + n % 2) % 2
                    src = (z * pp_size + y) * ep_size + ep
                    dst = (b1 * pp_size + x) * ep_size + c * 2 + b2
                    if src != dst:
                        pairs.append((src, dst))
        return pairs

    def device_body(w_gate, w_up, w_down, hot_ids):
        dtype = w_gate.dtype
        lay, exp_local, d_model, f_loc = w_gate.shape
        hot = hot_ids.shape[0]
        layers, f_all = lay * pp_size, f_loc * fs_size
        home = exp_local // (fs_size * pp_size)
        offset = jnp.clip(hot_ids - lax.axis_index("ep") * exp_local, 0, exp_local - 1)
        owner = hot_ids // exp_local
        picked = pick_hot(w_gate, w_up, w_down, offset)
        dma = pltpu.SemaphoreType.DMA
        buf13 = pltpu.VMEM((4, d_model, f_loc), dtype)
        buf2 = pltpu.VMEM((2, f_loc, d_model), dtype)
        shape = lambda *dims: jax.ShapeDtypeStruct(dims, dtype)
        tail_rows = f_loc * 2 // 3
        held = pltpu.VMEM((4, tail_rows, d_model), dtype)
        o13, o2, o2b, h13, h2, *tail = pl.pallas_call(
            move_kernel,
            out_shape=[
                shape(layers, home, d_model, 2 * f_all),
                shape(layers, f_all, d_model),
                shape(layers, f_all - fs_size * tail_rows, d_model),
                shape(layers, hot, d_model, 2 * f_all),
                shape(layers, hot, f_all, d_model),
            ] + [shape(tail_rows, d_model)] * 4,
            in_specs=[pl.BlockSpec(memory_space=pltpu.SMEM)] + [ANY] * 6,
            out_specs=[ANY] * 9,
            scratch_shapes=[
                buf13, buf2, buf13, buf2, buf13, buf2, held, dma((2, 4)),
                dma((3, 8)), dma((3, 2, 4)), dma((6,)), dma((6,)), dma((6,)), dma((6,)), dma((6,)),
                dma((3, 6)), dma((3, 6)), dma((4,)), dma((4, 6)), dma((4, 6)), dma((6,)),
            ],
            compiler_params=pltpu.CompilerParams(has_side_effects=True, vmem_limit_bytes=48 * 1024 * 1024),
        )(owner, w_gate, w_up, w_down, *picked)
        moved = [lax.ppermute(t, ("fs", "pp", "ep"), tail_pairs(n)) for n, t in enumerate(tail)]
        copied = 4 * (o13.size + o2.size + h13.size + h2.size)
        q13, q2, g13, g2 = pl.pallas_call(
            settle_kernel,
            out_shape=[
                shape(*o13.shape), shape(layers, home, f_all, d_model), shape(*h13.shape), shape(*h2.shape),
            ],
            in_specs=[ANY] * 5,
            out_specs=[ANY] * 4,
            scratch_shapes=[
                pltpu.VMEM((12, 512, 2 * f_all), dtype), pltpu.VMEM((12, f_loc, d_model), dtype), dma((2, 2, 12)),
            ],
            cost_estimate=pl.CostEstimate(flops=10**9, bytes_accessed=copied, transcendentals=0),
            compiler_params=pltpu.CompilerParams(vmem_limit_bytes=48 * 1024 * 1024),
        )(o13, o2, o2b, h13, h2)
        q2 = pl.pallas_call(
            place_kernel,
            out_shape=shape(*q2.shape),
            in_specs=[ANY] * 7,
            out_specs=ANY,
            scratch_shapes=[held, dma((2, 4))],
            input_output_aliases={6: 0},
            compiler_params=pltpu.CompilerParams(vmem_limit_bytes=56 * 1024 * 1024),
        )(tail[0], tail[1], *moved, q2)
        return q13, q2, g13, g2

    return jax.shard_map(
        device_body,
        mesh=mesh,
        in_specs=(in_spec, in_spec, down_spec, P()),
        out_specs=(home_spec, home_spec, P(), P()),
        check_vma=False,
    )
```

```python
import functools

import jax
import jax.numpy as jnp
from jax import lax
from jax.experimental import pallas as pl
from jax.experimental.pallas import tpu as pltpu
from jax.sharding import PartitionSpec as P

MESH = pl.DeviceIdType.MESH
ANY = pl.BlockSpec(memory_space=pl.ANY)


def move_kernel(
    owner_ref, off_ref, wg, wu, wd, o13, o2, o2b, h13, h2, t0, t1, t2, t3,
    all13, all2, give13, give2, own13, own2, par13, par2, far13, far2, t_sem,
    rg_send, rg_recv, loc_sem, dd_send, dd_recv, x_send, x_recv,
    n_send, n_recv, q_send, q_recv, w_sem,
):
    z = lax.axis_index("fs")
    y = lax.axis_index("pp")
    ep = lax.axis_index("ep")
    x, c = ep // 2, ep % 2
    d_model, f_loc = wg.shape[2], wg.shape[3]
    f_all = f_loc * 2
    tail_rows = t0.shape[0]
    kept = f_loc - tail_rows
    partner = (z, y, x * 2 + 1 - c)
    x_nbr = (z, y, (1 - x) * 2 + c)
    y_nbr = (z, 1 - y, ep)
    z_nbr = (1 - z, y, ep)

    def cols(half, up):
        return pl.ds(pl.multiple_of(half * f_loc + up * f_all, 128), f_loc)

    def remote(src, dst, send, recv, dev):
        return pltpu.make_async_remote_copy(
            src_ref=src, dst_ref=dst, send_sem=send, recv_sem=recv, device_id=dev, device_id_type=MESH
        )

    def vmem(b13, b2, k):
        return b2.at[k // 3] if k % 3 == 2 else b13.at[(k // 3) * 2 + k % 3]

    def hot_at(h, lay, half, w):
        if w == 2:
            return h2.at[lay, h, pl.ds(pl.multiple_of(half * f_loc, 128), f_loc)]
        return h13.at[lay, h, :, cols(half, w)]

    stays = (x == y) & (c == x)

    def home_refs(j, i, b0, w):
        b1, b2 = (z + i) % 2, (c + j) % 2
        src = (wg, wu, wd)[w].at[0, 4 * b2 + 2 * b1 + b0]
        if w == 2 and b0 == 1:
            src = src.at[pl.ds(tail_rows, kept)]
            dst = o2b.at[y, pl.ds(pl.multiple_of(z * kept, 128), kept)]
        elif w == 2:
            dst = o2.at[y, pl.ds(pl.multiple_of(z * f_loc, 128), f_loc)]
        else:
            dst = o13.at[y, b0, :, cols(z, w)]
        return src, dst, rg_recv.at[w, b0, y * 2 + z], (b1, x, c * 2 + b2)

    def home_copy(j, i, b0, w):
        src, dst, recv, dev = home_refs(j, i, b0, w)
        return remote(src, dst, rg_send.at[w, 4 * j + 2 * i + b0], recv, dev)

    def home_start(j, i, b0, w):
        if (j, i) != (0, 0):
            home_copy(j, i, b0, w).start()
            return

        @pl.when(stays)
        def _():
            src, dst, recv, _ = home_refs(j, i, b0, w)
            pltpu.make_async_copy(src, dst, recv).start()

        @pl.when(jnp.logical_not(stays))
        def _():
            home_copy(j, i, b0, w).start()

    def home_sent(j, i, b0, w):
        if (j, i) != (0, 0):
            home_copy(j, i, b0, w).wait_send()
            return

        @pl.when(jnp.logical_not(stays))
        def _():
            home_copy(j, i, b0, w).wait_send()

    homes = [
        (j, i, b0, w)
        for b0 in range(2) for w in range(3) for j in range(2) for i in range(2)
    ]

    tails = []
    for n in range(4):
        e = 4 * ((c + y + n % 2) % 2) + 2 * ((z + n // 2) % 2) + 1
        tails.append(pltpu.make_async_copy(wd.at[0, e, pl.ds(0, tail_rows)], (t0, t1, t2, t3)[n], t_sem.at[n]))

    CH = range(6)
    ORDER = (0, 3, 2, 5, 1, 4)
    dd = [remote(vmem(give13, give2, k), vmem(par13, par2, k), dd_send.at[k], dd_recv.at[k], partner) for k in CH]
    xs = [remote(vmem(own13, own2, k), vmem(far13, far2, k), x_send.at[k], x_recv.at[k], x_nbr) for k in CH]

    def choose(take_a, a, b, out):
        rows = a.shape[0] // 8

        def body(i, carry):
            at = pl.ds(pl.multiple_of(i * rows, 16), rows)
            out[at, :] = jnp.where(take_a, a[at, :], b[at, :])
            return carry

        lax.fori_loop(0, 8, body, 0)

    def take(held, h, out):
        rows = out.shape[0] // 8

        def body(i, carry):
            at = pl.ds(pl.multiple_of(i * rows, 16), rows)
            out[at, :] = held[off_ref[h], at, :]
            return carry

        lax.fori_loop(0, 8, body, 0)

    def take_all(w):
        held = all2 if w == 2 else all13
        for k in (w, 3 + w):
            take(held, 2 * (1 - c) + k // 3, vmem(give13, give2, k))
            take(held, 2 * c + k // 3, vmem(own13, own2, k))

    gates = pltpu.make_async_copy(wg.at[0], all13, loc_sem.at[0])
    ups = pltpu.make_async_copy(wu.at[0], all13, loc_sem.at[1])
    downs = pltpu.make_async_copy(wd.at[0], all2, loc_sem.at[2])
    gates.start()
    for b in homes[:2]:
        home_start(*b)
    downs.start()
    gates.wait()
    take_all(0)
    ups.start()
    downs.wait()
    take_all(2)
    for k in (0, 3):
        dd[k].start()
    ups.wait()
    take_all(1)
    for k in (2, 5):
        dd[k].start()
    for copy in tails:
        copy.start()
    for k in (1, 4):
        dd[k].start()

    for n in CH:
        k = ORDER[n]
        dd[k].wait_recv()
        owner = owner_ref[2 * c + k // 3]
        choose(owner % 2 == c, vmem(own13, own2, k), vmem(par13, par2, k), vmem(own13, own2, k))
        if n > 0:
            xs[ORDER[n - 1]].start()
    for b in homes[2:4]:
        home_start(*b)
    xs[ORDER[5]].start()
    for b in homes[4:]:
        home_start(*b)

    def hot_of(k):
        return 2 * c + k // 3

    def fan(k):
        src, w = vmem(par13, par2, k), k % 3
        dst = hot_at(hot_of(k), y, z, w)
        return (
            remote(src, dst, n_send.at[0, k], n_recv.at[0, k], y_nbr),
            remote(src, dst, n_send.at[1, k], n_recv.at[1, k], z_nbr),
            remote(src, dst, q_send.at[0, k], q_recv.at[0, k], partner),
            pltpu.make_async_copy(src, dst, w_sem.at[k]),
        )

    def from_y(k):
        at = hot_at(hot_of(k), 1 - y, z, k % 3)
        return at, remote(at, at, q_send.at[1, k], q_recv.at[1, k], partner)

    def from_z(k):
        at = hot_at(hot_of(k), y, 1 - z, k % 3)
        return at, remote(at, at, q_send.at[2, k], q_recv.at[2, k], partner)

    def onward(k):
        if k % 2 == 0:
            at = hot_at(hot_of(k), 1 - y, z, k % 3)
            return remote(at, at, n_send.at[2, k], n_recv.at[2, k], z_nbr)
        at = hot_at(hot_of(k), y, 1 - z, k % 3)
        return remote(at, at, n_send.at[2, k], n_recv.at[2, k], y_nbr)

    def from_diag(k):
        at = hot_at(hot_of(k), 1 - y, 1 - z, k % 3)
        return at, remote(at, at, q_send.at[3, k], q_recv.at[3, k], partner)

    def landed(at, sem):
        pltpu.make_async_copy(at, at, sem).wait()

    for n in CH:
        k = ORDER[n]
        xs[k].wait_recv()
        owner = owner_ref[2 * c + k // 3]
        choose(owner // 2 == x, vmem(own13, own2, k), vmem(far13, far2, k), vmem(par13, par2, k))
        if n > 0:
            for copy in fan(ORDER[n - 1]):
                copy.start()
    for k in CH:
        xs[k].wait_send()
    for copy in fan(ORDER[5]):
        copy.start()
    for k in ORDER:
        at, pass_on = from_y(k)
        landed(at, n_recv.at[0, k])
        if k % 2 == 0:
            onward(k).start()
        pass_on.start()
        at, pass_on = from_z(k)
        landed(at, n_recv.at[1, k])
        if k % 2 == 1:
            onward(k).start()
        pass_on.start()
    for k in ORDER:
        at, pass_on = from_diag(k)
        landed(at, n_recv.at[2, k])
        pass_on.start()

    for copy in tails:
        copy.wait()
    for k in CH:
        dd[k].wait_send()
        to_y, to_z, to_p, to_self = fan(k)
        to_y.wait_send()
        to_z.wait_send()
        to_p.wait_send()
        to_self.wait()
        onward(k).wait_send()
        from_y(k)[1].wait_send()
        from_z(k)[1].wait_send()
        from_diag(k)[1].wait_send()
    for k in CH:
        h, w = 2 * (1 - c) + k // 3, k % 3
        landed(hot_at(h, y, z, w), q_recv.at[0, k])
        landed(hot_at(h, 1 - y, z, w), q_recv.at[1, k])
        landed(hot_at(h, y, 1 - z, w), q_recv.at[2, k])
        landed(hot_at(h, 1 - y, 1 - z, w), q_recv.at[3, k])
    for b in homes:
        home_sent(*b)
    for w in range(3):
        for b0 in range(2):
            for lay in range(2):
                for half in range(2):
                    if w == 2 and b0 == 1:
                        at = o2b.at[lay, pl.ds(half * kept, kept)]
                    elif w == 2:
                        at = o2.at[lay, pl.ds(half * f_loc, f_loc)]
                    else:
                        at = o13.at[lay, b0, :, pl.ds(half * f_loc + w * f_all, f_loc)]
                    landed(at, rg_recv.at[w, b0, lay * 2 + half])


def settle_kernel(o13, o2, o2b, h13, h2, q13, q2, g13, g2, buf13, buf2, sems):
    slots = buf13.shape[0]
    rows13, rows2 = buf13.shape[1], buf2.shape[1]

    def tiles(src, dst, rows, buf):
        return [
            (src.at[pl.ds(r, rows)], dst.at[pl.ds(r, rows)], buf) for r in range(0, src.shape[0], rows)
        ]

    kept = o2b.shape[1] // 2

    work = []
    for lay in range(2):
        for n in range(o13.shape[1]):
            work += tiles(o13.at[lay, n], q13.at[lay, n], rows13, buf13)
        work += tiles(o2.at[lay], q2.at[lay, 0], rows2, buf2)
        for half in range(2):
            put = q2.at[lay, 1, pl.ds((half + 1) * rows2 - kept, kept)]
            work.append((o2b.at[lay, pl.ds(half * kept, kept)], put, buf2))
        for n in range(h13.shape[1]):
            work += tiles(h13.at[lay, n], g13.at[lay, n], rows13, buf13)
            work += tiles(h2.at[lay, n], g2.at[lay, n], rows2, buf2)

    used = {id(buf13): 0, id(buf2): 0}
    steps = []
    last = {}
    for src, dst, buf in work:
        kind = 0 if buf is buf13 else 1
        slot = used[id(buf)] % slots
        used[id(buf)] += 1
        before = last.get((kind, slot))
        tile = buf.at[slot, pl.ds(0, src.shape[0])]
        step = (
            pltpu.make_async_copy(src, tile, sems.at[kind, 0, slot]),
            pltpu.make_async_copy(tile, dst, sems.at[kind, 1, slot]),
            before,
        )
        last[kind, slot] = step
        steps.append(step)
    lag = slots // 2
    for n in range(len(steps) + lag):
        if n < len(steps):
            load, _, before = steps[n]
            if before is not None:
                before[1].wait()
            load.start()
        if n >= lag:
            load, store, _ = steps[n - lag]
            load.wait()
            store.start()
    for step in last.values():
        step[1].wait()


def place_kernel(t0, t1, r0, r1, r2, r3, q2_in, q2, buf, sems):
    z = lax.axis_index("fs")
    y = lax.axis_index("pp")
    ep = lax.axis_index("ep")
    x, c = ep // 2, ep % 2
    f_loc, tail_rows = q2.shape[2] // 2, buf.shape[1]

    def each(n, what):
        source = (r0, r1, r2, r3)[n]
        if n >= 2:
            what(source)
            return
        here = (x == y) & (c == x) & (y == n)
        pl.when(here)(lambda: what((t0, t1)[n]))
        pl.when(jnp.logical_not(here))(lambda: what(source))

    def store(n):
        lay, half = (c + x + n % 2) % 2, (z + n // 2) % 2
        rows = pl.ds(pl.multiple_of(half * f_loc, 128), tail_rows)
        return pltpu.make_async_copy(buf.at[n], q2.at[lay, 1, rows], sems.at[1, n])

    for n in range(4):
        each(n, lambda src: pltpu.make_async_copy(src, buf.at[n], sems.at[0, n]).start())
    for n in range(4):
        pltpu.make_async_copy(r0, buf.at[n], sems.at[0, n]).wait()
        store(n).start()
    for n in range(4):
        store(n).wait()


def solution(mesh):
    fs_size, pp_size, ep_size = mesh.shape["fs"], mesh.shape["pp"], mesh.shape["ep"]
    in_spec = P("pp", "ep", None, "fs")
    down_spec = P("pp", "ep", "fs", None)
    home_spec = P(None, ("pp", "ep", "fs"), None, None)

    def tail_pairs(n):
        pairs = []
        for z in range(fs_size):
            for y in range(pp_size):
                for ep in range(ep_size):
                    x, c = ep // 2, ep % 2
                    b1, b2 = (z + n // 2) % 2, (c + y + n % 2) % 2
                    src = (z * pp_size + y) * ep_size + ep
                    dst = (b1 * pp_size + x) * ep_size + c * 2 + b2
                    if src != dst:
                        pairs.append((src, dst))
        return pairs

    def device_body(w_gate, w_up, w_down, hot_ids):
        dtype = w_gate.dtype
        lay, exp_local, d_model, f_loc = w_gate.shape
        hot = hot_ids.shape[0]
        layers, f_all = lay * pp_size, f_loc * fs_size
        home = exp_local // (fs_size * pp_size)
        offset = jnp.clip(hot_ids - lax.axis_index("ep") * exp_local, 0, exp_local - 1)
        owner = hot_ids // exp_local
        dma = pltpu.SemaphoreType.DMA
        buf13 = pltpu.VMEM((4, d_model, f_loc), dtype)
        buf2 = pltpu.VMEM((2, f_loc, d_model), dtype)
        shape = lambda *dims: jax.ShapeDtypeStruct(dims, dtype)
        tail_rows = f_loc * 2 // 3
        held = pltpu.VMEM((4, tail_rows, d_model), dtype)
        o13, o2, o2b, h13, h2, *tail = pl.pallas_call(
            move_kernel,
            out_shape=[
                shape(layers, home, d_model, 2 * f_all),
                shape(layers, f_all, d_model),
                shape(layers, f_all - fs_size * tail_rows, d_model),
                shape(layers, hot, d_model, 2 * f_all),
                shape(layers, hot, f_all, d_model),
            ] + [shape(tail_rows, d_model)] * 4,
            in_specs=[pl.BlockSpec(memory_space=pltpu.SMEM)] * 2 + [ANY] * 3,
            out_specs=[ANY] * 9,
            scratch_shapes=[
                pltpu.VMEM((exp_local, d_model, f_loc), dtype), pltpu.VMEM((exp_local, f_loc, d_model), dtype),
                buf13, buf2, buf13, buf2, buf13, buf2, buf13, buf2, dma((4,)),
                dma((3, 8)), dma((3, 2, 4)), dma((3,)), dma((6,)), dma((6,)), dma((6,)), dma((6,)),
                dma((3, 6)), dma((3, 6)), dma((4, 6)), dma((4, 6)), dma((6,)),
            ],
            compiler_params=pltpu.CompilerParams(has_side_effects=True, vmem_limit_bytes=67043328),
        )(owner, offset, w_gate, w_up, w_down)
        moved = [lax.ppermute(t, ("fs", "pp", "ep"), tail_pairs(n)) for n, t in enumerate(tail)]
        copied = 4 * (o13.size + o2.size + h13.size + h2.size)
        q13, q2, g13, g2 = pl.pallas_call(
            settle_kernel,
            out_shape=[
                shape(*o13.shape), shape(layers, home, f_all, d_model), shape(*h13.shape), shape(*h2.shape),
            ],
            in_specs=[ANY] * 5,
            out_specs=[ANY] * 4,
            scratch_shapes=[
                pltpu.VMEM((12, 512, 2 * f_all), dtype), pltpu.VMEM((12, f_loc, d_model), dtype), dma((2, 2, 12)),
            ],
            cost_estimate=pl.CostEstimate(flops=10**9, bytes_accessed=copied, transcendentals=0),
            compiler_params=pltpu.CompilerParams(vmem_limit_bytes=48 * 1024 * 1024),
        )(o13, o2, o2b, h13, h2)
        q2 = pl.pallas_call(
            place_kernel,
            out_shape=shape(*q2.shape),
            in_specs=[ANY] * 7,
            out_specs=ANY,
            scratch_shapes=[held, dma((2, 4))],
            input_output_aliases={6: 0},
            compiler_params=pltpu.CompilerParams(vmem_limit_bytes=56 * 1024 * 1024),
        )(tail[0], tail[1], *moved, q2)
        return q13, q2, g13, g2

    return jax.shard_map(
        device_body,
        mesh=mesh,
        in_specs=(in_spec, in_spec, down_spec, P()),
        out_specs=(home_spec, home_spec, P(), P()),
        check_vma=False,
    )
```

```python
import functools

import jax
import jax.numpy as jnp
from jax import lax
from jax.experimental import pallas as pl
from jax.experimental.pallas import tpu as pltpu
from jax.sharding import PartitionSpec as P

MESH = pl.DeviceIdType.MESH
ANY = pl.BlockSpec(memory_space=pl.ANY)


def move_kernel(
    owner_ref, off_ref, wg, wu, wd, o13, o2, o2b, h13, h2, t0, t1, t2, t3,
    all13, all2, give13, give2, own13, own2, par13, par2, far13, far2, t_sem,
    rg_send, rg_recv, loc_sem, dd_send, dd_recv, x_send, x_recv,
    n_send, n_recv, f_send, q_send, q_recv, w_sem,
):
    z = lax.axis_index("fs")
    y = lax.axis_index("pp")
    ep = lax.axis_index("ep")
    x, c = ep // 2, ep % 2
    d_model, f_loc = wg.shape[2], wg.shape[3]
    f_all = f_loc * 2
    tail_rows = t0.shape[0]
    kept = f_loc - tail_rows
    partner = (z, y, x * 2 + 1 - c)
    x_nbr = (z, y, (1 - x) * 2 + c)
    y_nbr = (z, 1 - y, ep)
    z_nbr = (1 - z, y, ep)

    def cols(half, up):
        return pl.ds(pl.multiple_of(half * f_loc + up * f_all, 128), f_loc)

    def remote(src, dst, send, recv, dev):
        return pltpu.make_async_remote_copy(
            src_ref=src, dst_ref=dst, send_sem=send, recv_sem=recv, device_id=dev, device_id_type=MESH
        )

    def vmem(b13, b2, k):
        return b2.at[k // 3] if k % 3 == 2 else b13.at[(k // 3) * 2 + k % 3]

    def hot_at(h, lay, half, w):
        if w == 2:
            return h2.at[lay, h, pl.ds(pl.multiple_of(half * f_loc, 128), f_loc)]
        return h13.at[lay, h, :, cols(half, w)]

    stays = (x == y) & (c == x)

    def home_refs(j, i, b0, w):
        b1, b2 = (z + i) % 2, (c + j) % 2
        src = (wg, wu, wd)[w].at[0, 4 * b2 + 2 * b1 + b0]
        if w == 2 and b0 == 1:
            src = src.at[pl.ds(tail_rows, kept)]
            dst = o2b.at[y, pl.ds(pl.multiple_of(z * kept, 128), kept)]
        elif w == 2:
            dst = o2.at[y, pl.ds(pl.multiple_of(z * f_loc, 128), f_loc)]
        else:
            dst = o13.at[y, b0, :, cols(z, w)]
        return src, dst, rg_recv.at[w, b0, y * 2 + z], (b1, x, c * 2 + b2)

    def home_copy(j, i, b0, w):
        src, dst, recv, dev = home_refs(j, i, b0, w)
        return remote(src, dst, rg_send.at[w, 4 * j + 2 * i + b0], recv, dev)

    def home_start(j, i, b0, w):
        if (j, i) != (0, 0):
            home_copy(j, i, b0, w).start()
            return

        @pl.when(stays)
        def _():
            src, dst, recv, _ = home_refs(j, i, b0, w)
            pltpu.make_async_copy(src, dst, recv).start()

        @pl.when(jnp.logical_not(stays))
        def _():
            home_copy(j, i, b0, w).start()

    def home_sent(j, i, b0, w):
        if (j, i) != (0, 0):
            home_copy(j, i, b0, w).wait_send()
            return

        @pl.when(jnp.logical_not(stays))
        def _():
            home_copy(j, i, b0, w).wait_send()

    homes = [
        (j, i, b0, w)
        for b0 in range(2) for w in range(3) for j in range(2) for i in range(2)
    ]

    tails = []
    for n in range(4):
        e = 4 * ((c + y + n % 2) % 2) + 2 * ((z + n // 2) % 2) + 1
        tails.append(pltpu.make_async_copy(wd.at[0, e, pl.ds(0, tail_rows)], (t0, t1, t2, t3)[n], t_sem.at[n]))

    CH = range(6)
    ORDER = (0, 3, 2, 5, 1, 4)
    dd = [remote(vmem(give13, give2, k), vmem(par13, par2, k), dd_send.at[k], dd_recv.at[k], partner) for k in CH]
    xs = [remote(vmem(own13, own2, k), vmem(far13, far2, k), x_send.at[k], x_recv.at[k], x_nbr) for k in CH]

    def choose(take_a, a, b, out):
        rows = a.shape[0] // 8

        def body(i, carry):
            at = pl.ds(pl.multiple_of(i * rows, 16), rows)
            out[at, :] = jnp.where(take_a, a[at, :], b[at, :])
            return carry

        lax.fori_loop(0, 8, body, 0)

    def take(held, h, out):
        rows = out.shape[0] // 8

        def body(i, carry):
            at = pl.ds(pl.multiple_of(i * rows, 16), rows)
            out[at, :] = held[off_ref[h], at, :]
            return carry

        lax.fori_loop(0, 8, body, 0)

    def take_all(w):
        held = all2 if w == 2 else all13
        for k in (w, 3 + w):
            take(held, 2 * (1 - c) + k // 3, vmem(give13, give2, k))
            take(held, 2 * c + k // 3, vmem(own13, own2, k))

    gates = pltpu.make_async_copy(wg.at[0], all13, loc_sem.at[0])
    ups = pltpu.make_async_copy(wu.at[0], all13, loc_sem.at[1])
    downs = pltpu.make_async_copy(wd.at[0], all2, loc_sem.at[2])
    gates.start()
    for b in homes[:2]:
        home_start(*b)
    downs.start()
    gates.wait()
    take_all(0)
    ups.start()
    downs.wait()
    take_all(2)
    for k in (0, 3):
        dd[k].start()
    ups.wait()
    take_all(1)
    for k in (2, 5):
        dd[k].start()
    for copy in tails:
        copy.start()
    for k in (1, 4):
        dd[k].start()

    for n in CH:
        k = ORDER[n]
        dd[k].wait_recv()
        owner = owner_ref[2 * c + k // 3]
        choose(owner % 2 == c, vmem(own13, own2, k), vmem(par13, par2, k), vmem(own13, own2, k))
        if n > 0:
            xs[ORDER[n - 1]].start()
    for b in homes[2:4]:
        home_start(*b)
    xs[ORDER[5]].start()
    for b in homes[4:]:
        home_start(*b)

    def hot_of(k):
        return 2 * c + k // 3

    def fan(k):
        src, w = vmem(par13, par2, k), k % 3
        dst = hot_at(hot_of(k), y, z, w)
        return (
            remote(src, dst, n_send.at[0, k], n_recv.at[0, k], y_nbr),
            remote(src, dst, n_send.at[1, k], n_recv.at[1, k], z_nbr),
            remote(src, dst, q_send.at[0, k], q_recv.at[0, k], partner),
            pltpu.make_async_copy(src, dst, w_sem.at[k]),
        )

    def from_y(k):
        at = hot_at(hot_of(k), 1 - y, z, k % 3)
        return at, remote(at, at, q_send.at[1, k], q_recv.at[1, k], partner)

    def from_z(k):
        at = hot_at(hot_of(k), y, 1 - z, k % 3)
        return at, remote(at, at, q_send.at[2, k], q_recv.at[2, k], partner)

    def onward(k):
        if k % 2 == 0:
            at = hot_at(hot_of(k), 1 - y, z, k % 3)
            return remote(at, at, n_send.at[2, k], n_recv.at[2, k], z_nbr)
        at = hot_at(hot_of(k), y, 1 - z, k % 3)
        return remote(at, at, n_send.at[2, k], n_recv.at[2, k], y_nbr)

    ACROSS = (0, 3)

    def across(k):
        at = hot_at(hot_of(k), 1 - y, 1 - z, k % 3)
        return remote(at, at, f_send.at[k], n_recv.at[2, k], x_nbr)

    def onward_do(k, what):
        if k in ACROSS:
            pl.when(c == x)(lambda: what(onward(k)))
        else:
            what(onward(k))

    def from_diag(k):
        at = hot_at(hot_of(k), 1 - y, 1 - z, k % 3)
        return at, remote(at, at, q_send.at[3, k], q_recv.at[3, k], partner)

    def landed(at, sem):
        pltpu.make_async_copy(at, at, sem).wait()

    for n in CH:
        k = ORDER[n]
        xs[k].wait_recv()
        owner = owner_ref[2 * c + k // 3]
        choose(owner // 2 == x, vmem(own13, own2, k), vmem(far13, far2, k), vmem(par13, par2, k))
        if n > 0:
            for copy in fan(ORDER[n - 1]):
                copy.start()
    for k in CH:
        xs[k].wait_send()
    for copy in fan(ORDER[5]):
        copy.start()
    for k in ORDER:
        at, pass_on = from_y(k)
        landed(at, n_recv.at[0, k])
        if k % 2 == 0:
            onward_do(k, lambda copy: copy.start())
        pass_on.start()
        at, pass_on = from_z(k)
        landed(at, n_recv.at[1, k])
        if k % 2 == 1:
            onward_do(k, lambda copy: copy.start())
        pass_on.start()
    for k in ORDER:
        at, pass_on = from_diag(k)
        landed(at, n_recv.at[2, k])
        if k in ACROSS:
            pl.when(c == x)(lambda: across(k).start())
        pass_on.start()

    for copy in tails:
        copy.wait()
    for k in CH:
        dd[k].wait_send()
        to_y, to_z, to_p, to_self = fan(k)
        to_y.wait_send()
        to_z.wait_send()
        to_p.wait_send()
        to_self.wait()
        onward_do(k, lambda copy: copy.wait_send())
        if k in ACROSS:
            pl.when(c == x)(lambda: across(k).wait_send())
        from_y(k)[1].wait_send()
        from_z(k)[1].wait_send()
        from_diag(k)[1].wait_send()
    for k in CH:
        h, w = 2 * (1 - c) + k // 3, k % 3
        landed(hot_at(h, y, z, w), q_recv.at[0, k])
        landed(hot_at(h, 1 - y, z, w), q_recv.at[1, k])
        landed(hot_at(h, y, 1 - z, w), q_recv.at[2, k])
        landed(hot_at(h, 1 - y, 1 - z, w), q_recv.at[3, k])
    for b in homes:
        home_sent(*b)
    for w in range(3):
        for b0 in range(2):
            for lay in range(2):
                for half in range(2):
                    if w == 2 and b0 == 1:
                        at = o2b.at[lay, pl.ds(half * kept, kept)]
                    elif w == 2:
                        at = o2.at[lay, pl.ds(half * f_loc, f_loc)]
                    else:
                        at = o13.at[lay, b0, :, pl.ds(half * f_loc + w * f_all, f_loc)]
                    landed(at, rg_recv.at[w, b0, lay * 2 + half])


def settle_kernel(o13, o2, o2b, h13, h2, q13, q2, g13, g2, buf13, buf2, sems):
    slots = buf13.shape[0]
    rows13, rows2 = buf13.shape[1], buf2.shape[1]

    def tiles(src, dst, rows, buf):
        return [
            (src.at[pl.ds(r, rows)], dst.at[pl.ds(r, rows)], buf) for r in range(0, src.shape[0], rows)
        ]

    kept = o2b.shape[1] // 2

    work = []
    for lay in range(2):
        for n in range(o13.shape[1]):
            work += tiles(o13.at[lay, n], q13.at[lay, n], rows13, buf13)
        work += tiles(o2.at[lay], q2.at[lay, 0], rows2, buf2)
        for half in range(2):
            put = q2.at[lay, 1, pl.ds((half + 1) * rows2 - kept, kept)]
            work.append((o2b.at[lay, pl.ds(half * kept, kept)], put, buf2))
        for n in range(h13.shape[1]):
            work += tiles(h13.at[lay, n], g13.at[lay, n], rows13, buf13)
            work += tiles(h2.at[lay, n], g2.at[lay, n], rows2, buf2)

    used = {id(buf13): 0, id(buf2): 0}
    steps = []
    last = {}
    for src, dst, buf in work:
        kind = 0 if buf is buf13 else 1
        slot = used[id(buf)] % slots
        used[id(buf)] += 1
        before = last.get((kind, slot))
        tile = buf.at[slot, pl.ds(0, src.shape[0])]
        step = (
            pltpu.make_async_copy(src, tile, sems.at[kind, 0, slot]),
            pltpu.make_async_copy(tile, dst, sems.at[kind, 1, slot]),
            before,
        )
        last[kind, slot] = step
        steps.append(step)
    lag = slots // 2
    for n in range(len(steps) + lag):
        if n < len(steps):
            load, _, before = steps[n]
            if before is not None:
                before[1].wait()
            load.start()
        if n >= lag:
            load, store, _ = steps[n - lag]
            load.wait()
            store.start()
    for step in last.values():
        step[1].wait()


def place_kernel(t0, t1, r0, r1, r2, r3, q2_in, q2, buf, sems):
    z = lax.axis_index("fs")
    y = lax.axis_index("pp")
    ep = lax.axis_index("ep")
    x, c = ep // 2, ep % 2
    f_loc, tail_rows = q2.shape[2] // 2, buf.shape[1]

    def each(n, what):
        source = (r0, r1, r2, r3)[n]
        if n >= 2:
            what(source)
            return
        here = (x == y) & (c == x) & (y == n)
        pl.when(here)(lambda: what((t0, t1)[n]))
        pl.when(jnp.logical_not(here))(lambda: what(source))

    def store(n):
        lay, half = (c + x + n % 2) % 2, (z + n // 2) % 2
        rows = pl.ds(pl.multiple_of(half * f_loc, 128), tail_rows)
        return pltpu.make_async_copy(buf.at[n], q2.at[lay, 1, rows], sems.at[1, n])

    for n in range(4):
        each(n, lambda src: pltpu.make_async_copy(src, buf.at[n], sems.at[0, n]).start())
    for n in range(4):
        pltpu.make_async_copy(r0, buf.at[n], sems.at[0, n]).wait()
        store(n).start()
    for n in range(4):
        store(n).wait()


def solution(mesh):
    fs_size, pp_size, ep_size = mesh.shape["fs"], mesh.shape["pp"], mesh.shape["ep"]
    in_spec = P("pp", "ep", None, "fs")
    down_spec = P("pp", "ep", "fs", None)
    home_spec = P(None, ("pp", "ep", "fs"), None, None)

    def tail_pairs(n):
        pairs = []
        for z in range(fs_size):
            for y in range(pp_size):
                for ep in range(ep_size):
                    x, c = ep // 2, ep % 2
                    b1, b2 = (z + n // 2) % 2, (c + y + n % 2) % 2
                    src = (z * pp_size + y) * ep_size + ep
                    dst = (b1 * pp_size + x) * ep_size + c * 2 + b2
                    if src != dst:
                        pairs.append((src, dst))
        return pairs

    def device_body(w_gate, w_up, w_down, hot_ids):
        dtype = w_gate.dtype
        lay, exp_local, d_model, f_loc = w_gate.shape
        hot = hot_ids.shape[0]
        layers, f_all = lay * pp_size, f_loc * fs_size
        home = exp_local // (fs_size * pp_size)
        offset = jnp.clip(hot_ids - lax.axis_index("ep") * exp_local, 0, exp_local - 1)
        owner = hot_ids // exp_local
        dma = pltpu.SemaphoreType.DMA
        buf13 = pltpu.VMEM((4, d_model, f_loc), dtype)
        buf2 = pltpu.VMEM((2, f_loc, d_model), dtype)
        shape = lambda *dims: jax.ShapeDtypeStruct(dims, dtype)
        tail_rows = f_loc * 2 // 3
        held = pltpu.VMEM((4, tail_rows, d_model), dtype)
        o13, o2, o2b, h13, h2, *tail = pl.pallas_call(
            move_kernel,
            out_shape=[
                shape(layers, home, d_model, 2 * f_all),
                shape(layers, f_all, d_model),
                shape(layers, f_all - fs_size * tail_rows, d_model),
                shape(layers, hot, d_model, 2 * f_all),
                shape(layers, hot, f_all, d_model),
            ] + [shape(tail_rows, d_model)] * 4,
            in_specs=[pl.BlockSpec(memory_space=pltpu.SMEM)] * 2 + [ANY] * 3,
            out_specs=[ANY] * 9,
            scratch_shapes=[
                pltpu.VMEM((exp_local, d_model, f_loc), dtype), pltpu.VMEM((exp_local, f_loc, d_model), dtype),
                buf13, buf2, buf13, buf2, buf13, buf2, buf13, buf2, dma((4,)),
                dma((3, 8)), dma((3, 2, 4)), dma((3,)), dma((6,)), dma((6,)), dma((6,)), dma((6,)),
                dma((3, 6)), dma((3, 6)), dma((6,)), dma((4, 6)), dma((4, 6)), dma((6,)),
            ],
            compiler_params=pltpu.CompilerParams(has_side_effects=True, vmem_limit_bytes=67043328),
        )(owner, offset, w_gate, w_up, w_down)
        moved = [lax.ppermute(t, ("fs", "pp", "ep"), tail_pairs(n)) for n, t in enumerate(tail)]
        copied = 4 * (o13.size + o2.size + h13.size + h2.size)
        q13, q2, g13, g2 = pl.pallas_call(
            settle_kernel,
            out_shape=[
                shape(*o13.shape), shape(layers, home, f_all, d_model), shape(*h13.shape), shape(*h2.shape),
            ],
            in_specs=[ANY] * 5,
            out_specs=[ANY] * 4,
            scratch_shapes=[
                pltpu.VMEM((12, 512, 2 * f_all), dtype), pltpu.VMEM((12, f_loc, d_model), dtype), dma((2, 2, 12)),
            ],
            cost_estimate=pl.CostEstimate(flops=10**9, bytes_accessed=copied, transcendentals=0),
            compiler_params=pltpu.CompilerParams(vmem_limit_bytes=48 * 1024 * 1024),
        )(o13, o2, o2b, h13, h2)
        q2 = pl.pallas_call(
            place_kernel,
            out_shape=shape(*q2.shape),
            in_specs=[ANY] * 7,
            out_specs=ANY,
            scratch_shapes=[held, dma((2, 4))],
            input_output_aliases={6: 0},
            compiler_params=pltpu.CompilerParams(vmem_limit_bytes=56 * 1024 * 1024),
        )(tail[0], tail[1], *moved, q2)
        return q13, q2, g13, g2

    return jax.shard_map(
        device_body,
        mesh=mesh,
        in_specs=(in_spec, in_spec, down_spec, P()),
        out_specs=(home_spec, home_spec, P(), P()),
        check_vma=False,
    )
```
